256 devices in a mesh: gx: 16 (over y_lo, x, core), gy: 16 (over z, y_hi).
Axes of the slice: x: 4, y: 4 (y_hi: 2, y_lo: 2; y = y_hi * 2 + y_lo), z: 8, core: 2. Of those that a mesh axis runs over, the one named last changes fastest.
Arguments:
- east_class: int32 [1024, 1024], P('gx', 'gy'), may hold values from 0 to 7
- south_class: int32 [1024, 1024], P('gx', 'gy'), may hold values from 0 to 7
- cond_table: float32 [8], replicated, may hold values from 0.5 to 4
- leakage: float32 [1024, 1024], P('gx', 'gy'), may hold values from 0.1 to 1
- pad_mask: int32 [1024, 1024], P('gx', 'gy'), may hold values 0 or 1
- load_current: float32 [1024, 1024, 256], P('gx', 'gy'), may hold values from -24 to 24
Outputs:
- potential: float32 [1024, 1024, 256], P('gx', 'gy')
The draws below stay inside these ranges and needn't reach their ends.
All inputs are finite; a program needn't handle non-finite values. No bound on the sum of `pad_mask` on one device may be relied on, other than what follows from the above.
Results may differ from the reference program's by a relative error of at most 0.00002.
Values sent between devices are 32-bit elements; how exact they have to be, the bound alone decides.
No kernel may reach another device: no remote copies, remote signals or barrier semaphores. Data moves between devices by JAX's collectives and lax.ppermute only.
A program may use at most 64 MiB of HBM per device.

```python
import math
import jax
import jax.numpy as jnp

CASES = 256
CLASSES = 8
ITERS = 4
NX = 1024
NY = 1024


def touch_ends(values, key, smallest, top_value):
    extent = values.shape
    spot = [jax.random.randint(jax.random.fold_in(key, axis), (), 0, extent[axis]) for axis in range(len(extent))]
    values = values.at[tuple(spot)].set(smallest)
    longest = extent.index(max(extent))
    spot[longest] = (spot[longest] + 1) % extent[longest]
    return values.at[tuple(spot)].set(top_value)


def shard_levels(stream_key, shape, pieces, smallest, high):
    gain, own = 1.0, jax.random.fold_in(stream_key, 6)
    for axis_at, shards_of in pieces:
        draws = jnp.exp(jax.random.uniform(jax.random.fold_in(own, axis_at), (shards_of,), jnp.float32, smallest / len(pieces), high / len(pieces)))
        gain = gain * jnp.repeat(draws, shape[axis_at] // shards_of).reshape([-1 if axis == axis_at else 1 for axis in range(len(shape))])
    return gain


def scatter_about(stream_key, dims, deviation, bound, split=(), kind=jnp.bfloat16):
    array = deviation * jax.random.normal(stream_key, dims, jnp.float32)
    if split:
        array = array * shard_levels(stream_key, dims, split, -0.22, 0.18)
    return jnp.clip(array, -bound, bound).astype(kind)


def setup_inputs(seed: int = 0) -> dict:
    streams_of = jax.random.split(jax.random.key(seed), 7)
    east_class = touch_ends(jax.random.randint(streams_of[0], (NX, NY), 0, CLASSES), jax.random.fold_in(streams_of[0], 1), 0, CLASSES - 1).astype(jnp.int32)
    south_class = touch_ends(jax.random.randint(streams_of[1], (NX, NY), 0, CLASSES), jax.random.fold_in(streams_of[1], 1), 0, CLASSES - 1).astype(jnp.int32)
    cond_table = jnp.clip(jnp.exp(jax.random.uniform(streams_of[2], (CLASSES,), jnp.float32, math.log(0.5), math.log(4.0))), 0.5, 4.0)
    leakage = jnp.clip(jnp.exp(math.log(1.0) - 2.3025851 * jax.random.uniform(streams_of[3], (NX, NY), jnp.float32) ** shard_levels(streams_of[3], (NX, NY), ((0, 16), (1, 16)), -0.2, 0.2)), 0.1, 1.0)
    pad_mask = touch_ends((jax.random.randint(streams_of[4], (NX, NY), 0, 8) < 1).astype(jnp.int32), jax.random.fold_in(streams_of[4], 1), 0, 1)
    load_current = scatter_about(streams_of[5], (NX, NY, CASES), 4.0, 24.0, ((0, 16), (1, 16)), jnp.float32)
    return dict(east_class=east_class, south_class=south_class, cond_table=cond_table, leakage=leakage, pad_mask=pad_mask, load_current=load_current)


PAD_GAIN = 8.0
SPECTRAL_BOUND = 0.995


def chebyshev_weights(total_steps):
    weights = [1.0]
    for position in range(1, total_steps):
        if position == 1:
            weights.append(1.0 / (1.0 - SPECTRAL_BOUND * SPECTRAL_BOUND / 2.0))
        else:
            weights.append(1.0 / (1.0 - SPECTRAL_BOUND * SPECTRAL_BOUND * weights[-1] / 4.0))
    return weights


def lookup(classes, cond_table):
    labels = jnp.arange(cond_table.shape[0], dtype=jnp.int32)
    matches = classes[:, :, None] == labels
    return jnp.sum(jnp.where(matches, cond_table, 0.0), axis=-1)


def reference(east_class, south_class, cond_table, leakage, pad_mask, load_current):
    east_cond = lookup(east_class, cond_table)
    south_cond = lookup(south_class, cond_table)
    pads = pad_mask.astype(jnp.float32)
    east_west = jnp.roll(east_cond, 1, 1)
    south_north = jnp.roll(south_cond, 1, 0)
    diagonal = east_cond + east_west + south_cond + south_north + (leakage + PAD_GAIN * pads)
    source = (PAD_GAIN * pads[:, :, None] - load_current) / diagonal[:, :, None]
    omegas = chebyshev_weights(ITERS)
    field = source
    previous = source
    for iteration in range(ITERS):
        neighbours = east_cond[:, :, None] * jnp.roll(field, -1, 1) + east_west[:, :, None] * jnp.roll(field, 1, 1)
        neighbours = neighbours + south_cond[:, :, None] * jnp.roll(field, -1, 0)
        neighbours = neighbours + south_north[:, :, None] * jnp.roll(field, 1, 0)
        jacobi_value = source + neighbours / diagonal[:, :, None]
        if iteration == 0:
            updated = jacobi_value
        else:
            updated = omegas[iteration] * (jacobi_value - previous) + previous
        previous, field = field, updated
    return field
```

```python
import jax
import jax.numpy as jnp
from jax import lax
from jax.experimental import pallas as pl
from jax.experimental.pallas import tpu as pltpu
from jax.sharding import PartitionSpec as P


PAD_GAIN = 8.0
SPECTRAL_BOUND = 0.995


SIDE = 64
ROWS = SIDE + 8
COLS = SIDE + 16
GX_MSG = 8 * SIDE + SIDE
GY_MSG = 8 * SIDE + 16
CORNER_MSG = 64 + 16
F32 = jnp.float32


def weights():
    b2 = SPECTRAL_BOUND * SPECTRAL_BOUND
    first = 1.0 / (1.0 - b2 / 2.0)
    second = 1.0 / (1.0 - b2 * first / 4.0)
    third = 1.0 / (1.0 - b2 * second / 4.0)
    return first, second, third


W1, W2, W3 = weights()
MIX = W3 + (1.0 - W3) * W1
TOP = W1 * W2 * W3


def lanes_of(shape):
    return lax.broadcasted_iota(jnp.int32, shape, 1)


def coefficients(te, ts, tx, k):
    east = te[k : k + 8, :]
    west = te[k - 1 : k + 7, :]
    south = ts[k : k + 8, :]
    north = pltpu.roll(south, 1, 1)
    ground = tx[k : k + 8, :]
    inverse = 1.0 / (east + west + south + north + ground)
    fixed = jnp.where(ground > 4.0, PAD_GAIN, 0.0) * inverse
    return east * inverse, west * inverse, south * inverse, north * inverse, fixed, inverse


def spread(values, lane):
    return jnp.broadcast_to(values[:, lane : lane + 1], (8, 128))


def set_factors(factors, coef, s, row, c):
    lane = row + 4
    for which in range(4):
        coef[which, row, c : c + 8, :] = spread(factors[which], lane)
    fixed, inverse = spread(factors[4], lane), spread(factors[5], lane)
    for half in range(2):
        s[half, row, c : c + 8, :] = fixed - s[half, row, c : c + 8, :] * inverse


def sweep(src, coef, first, last, columns, unroll, emit):
    for c in columns:

        def rows(base, count, c=c):
            above = [src[half, base - 1, c : c + 8, :] for half in range(2)]
            here = [src[half, base, c : c + 8, :] for half in range(2)]
            for step in range(count):
                row = base + step
                factor = [coef[which, row, c : c + 8, :] for which in range(4)]
                for half in range(2):
                    below = src[half, row + 1, c : c + 8, :]
                    total = factor[0] * src[half, row, c + 1 : c + 9, :] + factor[1] * src[half, row, c - 1 : c + 7, :]
                    total = total + (factor[2] * below + factor[3] * above[half])
                    emit(half, row, c, total, here[half])
                    above[half], here[half] = here[half], below

        full = (last - first) // unroll
        if full == 1:
            rows(first, unroll)
        elif full > 1:

            def trip(index, carry, rows=rows):
                rows(first + index * unroll, unroll)
                return carry

            lax.fori_loop(0, full, trip, 0)
        if first + full * unroll < last:
            rows(first + full * unroll, last - first - full * unroll)


def chain(s, x1, u, t, coef, store, spans, windows, unroll):
    def to_x1(half, row, c, total, here):
        x1[half, row, c : c + 8, :] = here + total

    def to_u(half, row, c, total, here):
        u[half, row, c : c + 8, :] = total

    def to_t(half, row, c, total, here):
        t[half, row, c : c + 8, :] = total

    def to_out(half, row, c, total, here):
        store(
            half,
            row,
            c,
            s[half, row, c : c + 8, :] + (MIX * u[half, row, c : c + 8, :] + TOP * total),
        )

    for src, emit, (first, last), columns in zip((s, x1, u, t), (to_x1, to_u, to_t, to_out), spans, windows):
        sweep(src, coef, first, last, columns, unroll, emit)


def pack_kernel(*refs):
    small, load = refs[:5], refs[5]
    to_right, to_left, to_down, to_up, te, ts, tx = refs[6:13]
    edge, sem_edge, sem_rows, sem_small = refs[18:]
    table, east_class, south_class, leakage, pad_mask = refs[13:18]
    edges, tops = [], []
    nodes = [pltpu.make_async_copy(source, target, sem_small.at[i]) for i, (source, target) in enumerate(zip(small, refs[13:18]))]
    for copy in nodes:
        copy.start()
    for side in range(2):
        for half in range(2):
            copy = pltpu.make_async_copy(
                load.at[:, pl.ds(side * (SIDE - 8), 8), pl.ds(half * 128, 128)], edge.at[side, half], sem_edge.at[side, half]
            )
            copy.start()
            edges.append(copy)
    for side, message in enumerate((to_up, to_down)):
        for half in range(2):
            for row in range(4):
                copy = pltpu.make_async_copy(
                    load.at[side * (SIDE - 4) + row, :, pl.ds(half * 128, 128)],
                    message.at[pl.ds((half * 4 + row) * SIDE, SIDE), :],
                    sem_rows.at[side, half, row],
                )
                copy.start()
                tops.append(copy)

    for copy in nodes:
        copy.wait()

    def look_up(classes):
        found = jnp.zeros((SIDE, SIDE), F32)
        for label in range(8):
            found = jnp.where(classes == label, table[label], found)
        return found

    zeros = jnp.zeros((SIDE, 128 - SIDE), F32)

    def turned(values):
        return pltpu.roll(jnp.concatenate([values.T, zeros], axis=1), 8, 1)

    east = turned(look_up(east_class[...]))
    south = turned(look_up(south_class[...]))
    ground = turned(leakage[...] + PAD_GAIN * pad_mask[...].astype(F32))
    for target, values in ((te, east), (ts, south), (tx, ground)):
        target[0:8, :] = jnp.zeros((8, 128), F32)
        target[8 : SIDE + 8, :] = values
        target[SIDE + 8 : SIDE + 16, :] = jnp.zeros((8, 128), F32)
    lane = lanes_of((SIDE, 128))

    def banded(shifts):
        first, second, third = [
            values if shift == 0 else pltpu.roll(values, shift, 1) for values, shift in zip((east, south, ground), shifts)
        ]
        return jnp.where(lane < 8, first, jnp.where(lane < 16, second, third))

    to_down[8 * SIDE :, :] = banded((64, 72, 80))
    to_up[8 * SIDE :, :] = banded((120, 0, 8))
    put_conductances(to_right, 8 * SIDE, te, ts, tx, SIDE + 3, SIDE + 4)
    put_conductances(to_left, 8 * SIDE, te, ts, tx, 8, 8)
    for copy in edges:
        copy.wait()
    for side, message in enumerate((to_left, to_right)):
        for half in range(2):
            for row in range(SIDE):
                base = (half * SIDE + row) * 4
                message[base : base + 4, :] = edge[side, half, row, side * 4 : side * 4 + 4, :]
    for copy in tops:
        copy.wait()


def put_conductances(message, base, te, ts, tx, first_east, first_other):
    message[base : base + 5, :] = te[first_east : first_east + 5, :]
    message[base + 5 : base + 9, :] = ts[first_other : first_other + 4, :]
    message[base + 9 : base + 13, :] = tx[first_other : first_other + 4, :]
    message[base + 13 : base + 16, :] = jnp.zeros((3, 128), F32)


def inner_kernel(te, ts, tx, load, s, x1, u, t, coef, out, done, sem_in, sem_out):
    chunk = SIDE // 4
    copies = []
    for part in range(4):
        for half in range(2):
            copy = pltpu.make_async_copy(
                load.at[pl.ds(part * chunk, chunk), :, pl.ds(half * 128, 128)],
                s.at[half, pl.ds(4 + part * chunk, chunk), pl.ds(8, SIDE), :],
                sem_in.at[part, half],
            )
            copy.start()
            copies.append(copy)
    blocks = [coefficients(te, ts, tx, 8 + 8 * block) for block in range(SIDE // 8)]
    for part in range(4):
        copies[2 * part].wait()
        copies[2 * part + 1].wait()
        for block in range(SIDE // 8):
            for row in range(part * chunk, part * chunk + chunk):
                if row:
                    set_factors(blocks[block], coef, s, row + 4, 8 + 8 * block)

    def store(half, row, c, value):
        done[half, row - 4, c - 8 : c, :] = value

    everything = range(8, SIDE + 8, 8)
    middle = range(16, SIDE, 8)
    spans = ((6, SIDE + 2), (7, SIDE + 1), (8, SIDE), (9, SIDE - 1))
    chain(s, x1, u, t, coef, store, spans, (everything, everything, everything, middle), 10)
    outs = []
    for half in range(2):
        copy = pltpu.make_async_copy(
            done.at[half, pl.ds(5, SIDE - 10), pl.ds(8, SIDE - 16), :],
            out.at[pl.ds(5, SIDE - 10), pl.ds(8, SIDE - 16), pl.ds(half * 128, 128)],
            sem_out.at[half],
        )
        copy.start()
        outs.append(copy)
    for copy in outs:
        copy.wait()


def corner_kernel(te, ts, tx, from_up, from_down, to_right, to_left, te2, ts2, tx2):
    lane = lanes_of((SIDE, 128))
    upper, lower = from_up[8 * SIDE :, :], from_down[8 * SIDE :, :]
    for source, target, down, up in ((te, te2, 0, 72), (ts, ts2, 120, 64), (tx, tx2, 112, 56)):
        head = pltpu.roll(upper, down, 1) if down else upper
        tail = pltpu.roll(lower, up, 1)
        own = source[8 : SIDE + 8, :]
        target[0:8, :] = jnp.zeros((8, 128), F32)
        target[8 : SIDE + 8, :] = jnp.where(lane < 8, head, jnp.where(lane < SIDE + 8, own, tail))
        target[SIDE + 8 : SIDE + 16, :] = jnp.zeros((8, 128), F32)
    for message, first in ((to_right, SIDE - 4), (to_left, 0)):
        for half in range(2):
            for row in range(8):
                origin = from_up if row < 4 else from_down
                base = (half * 8 + row) * 4
                at = (half * 4 + row % 4) * SIDE + first
                message[base : base + 4, :] = origin[at : at + 4, :]
    put_conductances(to_right, 64, te2, ts2, tx2, SIDE + 3, SIDE + 4)
    put_conductances(to_left, 64, te2, ts2, tx2, 8, 8)


def rows_kernel(te, ts, tx, from_up, from_down, own_up, *rest):
    s, x1, u, t, coef, out, done, sem_out = rest[6:]
    for half in range(2):
        for row in range(4):
            at = (half * 4 + row) * SIDE
            s[half, row, 8 : SIDE + 8, :] = from_up[at : at + SIDE, :]
            s[half, SIDE + 4 + row, 8 : SIDE + 8, :] = from_down[at : at + SIDE, :]
        s[half, 4, 8 : SIDE + 8, :] = own_up[half * 4 * SIDE : half * 4 * SIDE + SIDE, :]
    for block in range(SIDE // 8):
        factors = coefficients(te, ts, tx, 8 + 8 * block)
        for row in (0, 1, 2, 3, 4, SIDE + 4, SIDE + 5, SIDE + 6, SIDE + 7):
            set_factors(factors, coef, s, row, 8 + 8 * block)
    everything = range(8, SIDE + 8, 8)
    middle = range(16, SIDE, 8)
    windows = (everything, everything, everything, middle)
    outs = []
    for side, first in enumerate((1, SIDE + 2)):
        spans = tuple((first + shift, first + shift + 5) for shift in ((0, 1, 2, 3), (0, -1, -2, -3))[side])

        def store(half, row, c, value, side=side):
            done[half, row - 4 if side == 0 else row - (SIDE - 1) + 5, c - 8 : c, :] = value

        chain(s, x1, u, t, coef, store, spans, windows, 5)
        for half in range(2):
            copy = pltpu.make_async_copy(
                done.at[half, pl.ds(5 * side, 5), pl.ds(8, SIDE - 16), :],
                out.at[pl.ds(side * (SIDE - 5), 5), pl.ds(8, SIDE - 16), pl.ds(half * 128, 128)],
                sem_out.at[side, half],
            )
            copy.start()
            outs.append(copy)
    for copy in outs:
        copy.wait()


def sides_kernel(te2, ts2, tx2, from_up, from_down, own_left, from_left, from_right, corner_left, corner_right, *rest):
    s, x1, u, t, coef, out, te, ts, tx, done, sem_out = rest[6:]
    for source, target in ((te2, te), (ts2, ts), (tx2, tx)):
        target[...] = source[...]
    for main, corner, first_east, first_other in ((from_left, corner_left, 3, 4), (from_right, corner_right, SIDE + 8, SIDE + 8)):
        lane = lanes_of((16, 128))
        merged = jnp.where((lane >= 8) & (lane < SIDE + 8), main[8 * SIDE :, :], corner[64:, :])
        te[first_east : first_east + 5, :] = merged[0:5, :]
        ts[first_other : first_other + 4, :] = merged[5:9, :]
        tx[first_other : first_other + 4, :] = merged[9:13, :]
    outs = []
    for side, (main, corner, c) in enumerate(((from_left, corner_left, 1), (from_right, corner_right, SIDE + 8))):
        halo = 4 if side == 0 else SIDE + 8
        factors = coefficients(te, ts, tx, c)
        for row in range(ROWS):
            for half in range(2):
                if 4 <= row < SIDE + 4:
                    at = (half * SIDE + row - 4) * 4
                    s[half, row, halo : halo + 4, :] = main[at : at + 4, :]
                    if side == 0:
                        s[half, row, 8:9, :] = own_left[at : at + 1, :]
                else:
                    part = row if row < 4 else row - SIDE
                    at = (half * 8 + part) * 4
                    s[half, row, halo : halo + 4, :] = corner[at : at + 4, :]
                    if side == 0:
                        at = (half * 4 + part % 4) * SIDE
                        s[half, row, 8:9, :] = (from_up if row < 4 else from_down)[at : at + 1, :]
            set_factors(factors, coef, s, row, c)
        spans = ((1, SIDE + 7), (2, SIDE + 6), (3, SIDE + 5), (4, SIDE + 4))
        windows = ((4,), (5,), (6,), (8,)) if side == 0 else ((SIDE + 4,), (SIDE + 3,), (SIDE + 2,), (SIDE,))

        def store(half, row, c, value, side=side):
            done[side, half, row - 4, :, :] = value

        chain(s, x1, u, t, coef, store, spans, windows, 16)
        for half in range(2):
            copy = pltpu.make_async_copy(
                done.at[side, half],
                out.at[:, pl.ds(side * (SIDE - 8), 8), pl.ds(half * 128, 128)],
                sem_out.at[side, half],
            )
            copy.start()
            outs.append(copy)
    for copy in outs:
        copy.wait()


VMEM = pl.BlockSpec(memory_space=pltpu.VMEM)
HBM = pl.BlockSpec(memory_space=pltpu.HBM)
DMA = pltpu.SemaphoreType.DMA
FIELD = pltpu.VMEM((2, ROWS, COLS, 128), F32)
COEF = pltpu.VMEM((4, ROWS, COLS, 128), F32)
TURNED = pltpu.VMEM((COLS, 128), F32)
STATE = (FIELD, FIELD, FIELD, FIELD, COEF)


def call(kernel, in_specs, out_shape, out_specs, scratch, cost, grant, aliases=None):
    return pl.pallas_call(
        kernel,
        in_specs=in_specs,
        out_shape=out_shape,
        out_specs=out_specs,
        scratch_shapes=scratch,
        input_output_aliases=aliases or {},
        cost_estimate=pl.CostEstimate(flops=cost, bytes_accessed=1 << 20, transcendentals=0),
        compiler_params=pltpu.CompilerParams(vmem_limit_bytes=grant << 20),
    )


def block(east_class, south_class, cond_table, leakage, pad_mask, load):
    gx, gy = lax.axis_size("gx"), lax.axis_size("gy")

    def shift(values, axis, step):
        count = gx if axis == "gx" else gy
        return lax.ppermute(values, axis, [(i, (i + step) % count) for i in range(count)])

    potential = pltpu.HBM((SIDE, SIDE, 256), F32)
    given = [pltpu.with_memory_space_constraint(a, pltpu.HBM) for a in (cond_table, east_class, south_class, leakage, pad_mask, load)]
    to_right, to_left, to_down, to_up, te, ts, tx = call(
        pack_kernel,
        [HBM] * 6,
        [pltpu.VMEM((GY_MSG, 128), F32)] * 2 + [pltpu.VMEM((GX_MSG, 128), F32)] * 2 + [TURNED] * 3,
        [VMEM] * 7,
        [pltpu.SMEM((8,), F32)]
        + [pltpu.VMEM((SIDE, SIDE), kind) for kind in (jnp.int32, jnp.int32, F32, jnp.int32)]
        + [pltpu.VMEM((2, 2, SIDE, 8, 128), F32), DMA((2, 2)), DMA((2, 2, 4)), DMA((5,))],
        1 << 22,
        4,
    )(*given)
    from_left = shift(to_right, "gy", 1)
    from_up = shift(to_down, "gx", 1)
    from_down = shift(to_up, "gx", -1)
    from_right = shift(to_left, "gy", -1)
    *state, out = call(
        inner_kernel,
        [VMEM] * 3 + [HBM],
        [*STATE, potential],
        [VMEM] * 5 + [HBM],
        [pltpu.VMEM((2, SIDE, SIDE, 128), F32), DMA((4, 2)), DMA((2,))],
        1 << 25,
        6,
    )(te, ts, tx, given[5])
    corner_right, corner_left, te2, ts2, tx2 = call(
        corner_kernel, [VMEM] * 5, [pltpu.VMEM((CORNER_MSG, 128), F32)] * 2 + [TURNED] * 3, [VMEM] * 5, [], 1 << 20, 4
    )(te, ts, tx, from_up, from_down)
    corner_from_left = shift(corner_right, "gy", 1)
    corner_from_right = shift(corner_left, "gy", -1)
    *state, out = call(
        rows_kernel,
        [VMEM] * 11 + [HBM],
        [*STATE, potential],
        [VMEM] * 5 + [HBM],
        [pltpu.VMEM((2, 10, SIDE, 128), F32), DMA((2, 2))],
        1 << 24,
        4,
        {6 + i: i for i in range(6)},
    )(te2, ts2, tx2, from_up, from_down, to_up, *state, out)
    *state, out = call(
        sides_kernel,
        [VMEM] * 15 + [HBM],
        [*STATE, potential],
        [VMEM] * 5 + [HBM],
        [TURNED] * 3 + [pltpu.VMEM((2, 2, SIDE, 8, 128), F32), DMA((2, 2))],
        1 << 24,
        4,
        {10 + i: i for i in range(6)},
    )(te2, ts2, tx2, from_up, from_down, to_left, from_left, from_right, corner_from_left, corner_from_right, *state, out)
    return out


def solution(mesh):
    in_specs = (P("gx", "gy"), P("gx", "gy"), P(), P("gx", "gy"), P("gx", "gy"), P("gx", "gy", None))
    return jax.shard_map(block, mesh=mesh, in_specs=in_specs, out_specs=P("gx", "gy", None), check_vma=False)
```

```python
import jax
import jax.numpy as jnp
from jax import lax
from jax.experimental import pallas as pl
from jax.experimental.pallas import tpu as pltpu
from jax.sharding import PartitionSpec as P


PAD_GAIN = 8.0
SPECTRAL_BOUND = 0.995


SIDE = 64
ROWS = SIDE + 8
COLS = SIDE + 16
GX_MSG = 8 * SIDE + SIDE
GY_MSG = 8 * SIDE
CORNER_MSG = 24 + 16
TURNED_ROWS = SIDE + 24
F32 = jnp.float32


def weights():
    b2 = SPECTRAL_BOUND * SPECTRAL_BOUND
    first = 1.0 / (1.0 - b2 / 2.0)
    second = 1.0 / (1.0 - b2 * first / 4.0)
    third = 1.0 / (1.0 - b2 * second / 4.0)
    return first, second, third


W1, W2, W3 = weights()
MIX = W3 + (1.0 - W3) * W1
TOP = W1 * W2 * W3


EAST, SOUTH, ROOT, FIXED = range(4)


def lanes_of(shape):
    return lax.broadcasted_iota(jnp.int32, shape, 1)


def turn_factors(te, ts, tx, factors, roots, easts, souths):
    for k in roots:
        south = ts[k : k + 8, :]
        ground = tx[k : k + 8, :]
        diagonal = te[k : k + 8, :] + te[k - 1 : k + 7, :] + south + pltpu.roll(south, 1, 1) + ground
        root = 1.0 / jnp.sqrt(diagonal)
        factors[ROOT, k : k + 8, :] = root
        factors[FIXED, k : k + 8, :] = jnp.where(ground > 4.0, PAD_GAIN, 0.0) * root
    for k in easts:
        factors[EAST, k : k + 8, :] = te[k : k + 8, :] * factors[ROOT, k : k + 8, :] * factors[ROOT, k + 1 : k + 9, :]
    for k in souths:
        root = factors[ROOT, k : k + 8, :]
        factors[SOUTH, k : k + 8, :] = ts[k : k + 8, :] * root * pltpu.roll(root, 127, 1)


def spread(values, lane):
    return jnp.broadcast_to(values[:, lane : lane + 1], (8, 128))


def to_source(s, row, c, fixed, root):
    for half in range(2):
        s[half, row, pl.ds(c, 8), :] = fixed - s[half, row, pl.ds(c, 8), :] * root


def neighbours(src, coef, base, count, c, emit):
    above = [src[half, base - 1, pl.ds(c, 8), :] for half in range(2)]
    here = [src[half, base, pl.ds(c, 8), :] for half in range(2)]
    north = coef[SOUTH, base - 1, pl.ds(c, 8), :]
    for step in range(count):
        row = base + step
        east = coef[EAST, row, pl.ds(c, 8), :]
        west = coef[EAST, row, pl.ds(c - 1, 8), :]
        south = coef[SOUTH, row, pl.ds(c, 8), :]
        for half in range(2):
            below = src[half, row + 1, pl.ds(c, 8), :]
            total = east * src[half, row, pl.ds(c + 1, 8), :] + west * src[half, row, pl.ds(c - 1, 8), :]
            total = total + (south * below + north * above[half])
            emit(half, row, c, total, here[half])
            above[half], here[half] = here[half], below
        north = south


def sweep(src, coef, first, last, columns, unroll, emit):
    full = (last - first) // unroll
    for c in columns:
        if full == 1:
            neighbours(src, coef, first, unroll, c, emit)
        elif full > 1:

            def trip(index, carry, c=c):
                neighbours(src, coef, first + index * unroll, unroll, c, emit)
                return carry

            lax.fori_loop(0, full, trip, 0)
        if first + full * unroll < last:
            neighbours(src, coef, first + full * unroll, last - first - full * unroll, c, emit)


def adding(target):
    def emit(half, row, c, total, here):
        target[half, row, pl.ds(c, 8), :] = here + total

    return emit


def placing(target):
    def emit(half, row, c, total, here):
        target[half, row, pl.ds(c, 8), :] = total

    return emit


def result(s, u, coef, half, row, c, total):
    value = s[half, row, pl.ds(c, 8), :] + (MIX * u[half, row, pl.ds(c, 8), :] + TOP * total)
    return value * coef[ROOT, row, pl.ds(c, 8), :]


def pack_kernel(*refs):
    small, load = refs[:5], refs[5]
    to_right, to_left, to_down, to_up, te, ts, tx = refs[6:13]
    edge, sem_edge, sem_rows, sem_small = refs[18:]
    table, east_class, south_class, leakage, pad_mask = refs[13:18]
    edges, tops = [], []
    nodes = [pltpu.make_async_copy(source, target, sem_small.at[i]) for i, (source, target) in enumerate(zip(small, refs[13:18]))]
    for copy in nodes:
        copy.start()
    for side in range(2):
        for half in range(2):
            copy = pltpu.make_async_copy(
                load.at[:, pl.ds(side * (SIDE - 8), 8), pl.ds(half * 128, 128)], edge.at[side, half], sem_edge.at[side, half]
            )
            copy.start()
            edges.append(copy)
    for side, message in enumerate((to_up, to_down)):
        for half in range(2):
            for row in range(4):
                copy = pltpu.make_async_copy(
                    load.at[side * (SIDE - 4) + row, :, pl.ds(half * 128, 128)],
                    message.at[pl.ds((half * 4 + row) * SIDE, SIDE), :],
                    sem_rows.at[side, half, row],
                )
                copy.start()
                tops.append(copy)

    for copy in nodes:
        copy.wait()

    def look_up(classes):
        found = jnp.zeros((SIDE, SIDE), F32)
        for label in range(8):
            found = jnp.where(classes == label, table[label], found)
        return found

    zeros = jnp.zeros((SIDE, 128 - SIDE), F32)

    def turned(values):
        return pltpu.roll(jnp.concatenate([values.T, zeros], axis=1), 8, 1)

    east = turned(look_up(east_class[...]))
    south = turned(look_up(south_class[...]))
    ground = turned(leakage[...] + PAD_GAIN * pad_mask[...].astype(F32))
    for target, values in ((te, east), (ts, south), (tx, ground)):
        target[0:8, :] = jnp.zeros((8, 128), F32)
        target[8 : SIDE + 8, :] = values
        target[SIDE + 8 :, :] = jnp.zeros((16, 128), F32)
    lane = lanes_of((SIDE, 128))

    def banded(shifts):
        first, second, third = [
            values if shift == 0 else pltpu.roll(values, shift, 1) for values, shift in zip((east, south, ground), shifts)
        ]
        return jnp.where(lane < 8, first, jnp.where(lane < 16, second, third))

    to_down[8 * SIDE :, :] = banded((64, 72, 80))
    to_up[8 * SIDE :, :] = banded((120, 0, 8))
    for copy in edges:
        copy.wait()
    for side, message in enumerate((to_left, to_right)):
        for half in range(2):
            for row in range(SIDE):
                base = (half * SIDE + row) * 4
                message[base : base + 4, :] = edge[side, half, row, side * 4 : side * 4 + 4, :]
    for copy in tops:
        copy.wait()


def put_conductances(message, base, te, ts, tx, first_east, first_other):
    message[base : base + 5, :] = te[first_east : first_east + 5, :]
    message[base + 5 : base + 9, :] = ts[first_other : first_other + 4, :]
    message[base + 9 : base + 13, :] = tx[first_other : first_other + 4, :]
    message[base + 13 : base + 16, :] = jnp.zeros((3, 128), F32)


def first_kernel(te, ts, tx, load, s, x1, coef, factors, sem):
    def part(group, half):
        return pltpu.make_async_copy(
            load.at[pl.ds(group * 8, 8), :, pl.ds(half * 128, 128)],
            s.at[half, pl.ds(4 + group * 8, 8), pl.ds(8, SIDE), :],
            sem.at[group, half],
        )

    for group in range(SIDE // 8):
        for half in range(2):
            part(group, half).start()
    own = range(8, SIDE + 8, 8)
    turn_factors(te, ts, tx, factors, own, own, own)

    def body(group, carry):
        for half in range(2):
            part(group, half).wait()
        for step in range(8):
            row = group * 8 + 4 + step
            for c in own:
                values = [spread(factors[which, c : c + 8, :], 8 + step) for which in range(4)]
                for which in (EAST, SOUTH, ROOT):
                    coef[which, row, c : c + 8, :] = values[which]
                to_source(s, row, c, values[FIXED], values[ROOT])
        for c in own:
            neighbours(s, coef, group * 8 + 3, 8, c, adding(x1))
            for which in range(4):
                factors[which, c : c + 8, :] = pltpu.roll(factors[which, c : c + 8, :], 120, 1)
        return carry

    lax.fori_loop(0, SIDE // 8, body, 0)


def corner_cells():
    for half in range(2):
        for side in range(2):
            for distance in (1, 2, 3):
                yield (half * 2 + side) * 6 + (0, 3, 5)[distance - 1], half, side, distance


def corner_kernel(te, ts, tx, from_up, from_down, to_right, to_left, te2, ts2, tx2):
    lane = lanes_of((SIDE, 128))
    upper, lower = from_up[8 * SIDE :, :], from_down[8 * SIDE :, :]
    for source, target, down, up in ((te, te2, 0, 72), (ts, ts2, 120, 64), (tx, tx2, 112, 56)):
        head = pltpu.roll(upper, down, 1) if down else upper
        tail = pltpu.roll(lower, up, 1)
        own = source[8 : SIDE + 8, :]
        target[0:8, :] = jnp.zeros((8, 128), F32)
        target[8 : SIDE + 8, :] = jnp.where(lane < 8, head, jnp.where(lane < SIDE + 8, own, tail))
        target[SIDE + 8 :, :] = jnp.zeros((16, 128), F32)
    for offset, half, side, distance in corner_cells():
        count = 4 - distance
        origin, row = (from_down, distance - 1) if side else (from_up, 4 - distance)
        at = (half * 4 + row) * SIDE
        to_right[offset : offset + count, :] = origin[at + SIDE - count : at + SIDE, :]
        to_left[offset : offset + count, :] = origin[at : at + count, :]
    put_conductances(to_right, 24, te2, ts2, tx2, SIDE + 3, SIDE + 4)
    put_conductances(to_left, 24, te2, ts2, tx2, 8, 8)


def main_kernel(te, ts, tx, from_up, from_down, own_up, *rest):
    s, x1, coef, u, t, out, factors, done, sem = rest[3:]
    own = range(8, SIDE + 8, 8)
    turn_factors(te, ts, tx, factors, own, own, own)
    for half in range(2):
        for row in range(4):
            at = (half * 4 + row) * SIDE
            s[half, row, 8 : SIDE + 8, :] = from_up[at : at + SIDE, :]
            s[half, SIDE + 4 + row, 8 : SIDE + 8, :] = from_down[at : at + SIDE, :]
        s[half, 4, 8 : SIDE + 8, :] = own_up[half * 4 * SIDE : half * 4 * SIDE + SIDE, :]
    for row in (0, 1, 2, 3, 4, SIDE + 3, SIDE + 4, SIDE + 5, SIDE + 6, SIDE + 7):
        for c in own:
            values = [spread(factors[which, c : c + 8, :], row + 4) for which in range(4)]
            for which in (EAST, SOUTH, ROOT):
                coef[which, row, c : c + 8, :] = values[which]
            if row != SIDE + 3:
                to_source(s, row, c, values[FIXED], values[ROOT])
    sweep(s, coef, 1, 6, own, 5, adding(x1))
    sweep(s, coef, SIDE + 3, SIDE + 7, own, 4, adding(x1))
    sweep(x1, coef, 2, SIDE + 6, own, 17, placing(u))
    sweep(u, coef, 3, SIDE + 5, own, 22, placing(t))

    def finish(half, row, c, total, here):
        done[half, row - 4, c - 8 : c, :] = result(s, u, coef, half, row, c, total)

    outs = []
    for part in range(4):
        rows = pl.ds(part * 16, 16)
        sweep(t, coef, 4 + part * 16, 20 + part * 16, range(16, SIDE, 8), 16, finish)
        for half in range(2):
            copy = pltpu.make_async_copy(
                done.at[half, rows, pl.ds(8, SIDE - 16), :],
                out.at[rows, pl.ds(8, SIDE - 16), pl.ds(half * 128, 128)],
                sem.at[part, half],
            )
            copy.start()
            outs.append(copy)
    for copy in outs:
        copy.wait()


def sides_kernel(te2, ts2, tx2, from_up, from_down, own_left, from_left, from_right, corner_left, corner_right, *rest):
    s, x1, coef, u, t, out, te, ts, tx, factors, done, sem = rest[6:]
    for source, target in ((te2, te), (ts2, ts), (tx2, tx)):
        target[...] = source[...]
    for corner, first_east, first_other in ((corner_left, 3, 4), (corner_right, SIDE + 8, SIDE + 8)):
        te[first_east : first_east + 5, :] = corner[24:29, :]
        ts[first_other : first_other + 4, :] = corner[29:33, :]
        tx[first_other : first_other + 4, :] = corner[33:37, :]
    turn_factors(te, ts, tx, factors, (1, 8, SIDE, SIDE + 8), (1, SIDE + 7), (1, SIDE + 8))

    def unpack(index, carry):
        for step in range(8):
            row = index * 8 + step
            for half in range(2):
                at = (half * SIDE + row) * 4
                s[half, row + 4, 4:8, :] = from_left[pl.ds(at, 4), :]
                s[half, row + 4, 8:9, :] = own_left[pl.ds(at, 1), :]
                s[half, row + 4, SIDE + 8 : SIDE + 12, :] = from_right[pl.ds(at, 4), :]
        return carry

    lax.fori_loop(0, SIDE // 8, unpack, 0)
    for half in range(2):
        for row in range(4):
            at = (half * 4 + row) * SIDE
            s[half, row, 8:9, :] = from_up[at : at + 1, :]
            s[half, SIDE + 4 + row, 8:9, :] = from_down[at : at + 1, :]
    for offset, half, side, distance in corner_cells():
        count = 4 - distance
        row = SIDE + 3 + distance if side else 4 - distance
        s[half, row, 8 - count : 8, :] = corner_left[offset : offset + count, :]
        s[half, row, SIDE + 8 : SIDE + 8 + count, :] = corner_right[offset : offset + count, :]
    used = [(which, 1) for which in range(4)] + [(EAST, SIDE + 7)] + [(which, SIDE + 8) for which in (SOUTH, ROOT, FIXED)]

    def body(group, carry):
        for step in range(8):
            row = group * 8 + step
            values = [spread(factors[which, c : c + 8, :], 4 + step) for which, c in used]
            for (which, c), value in zip(used, values):
                if which != FIXED:
                    coef[which, row, c : c + 8, :] = value
            to_source(s, row, 1, values[FIXED], values[ROOT])
            to_source(s, row, SIDE + 8, values[7], values[6])
        for which, c in used:
            factors[which, c : c + 8, :] = pltpu.roll(factors[which, c : c + 8, :], 120, 1)
        return carry

    lax.fori_loop(0, ROWS // 8, body, 0)
    sweep(s, coef, 1, SIDE + 7, (4, SIDE + 4), 14, adding(x1))
    sweep(x1, coef, 2, SIDE + 6, (5, SIDE + 3), 17, placing(u))
    sweep(u, coef, 3, SIDE + 5, (6, SIDE + 2), 22, placing(t))
    outs = []
    for side in range(2):

        def finish(half, row, c, total, here, side=side):
            done[side, half, row - 4, :, :] = result(s, u, coef, half, row, c, total)

        sweep(t, coef, 4, SIDE + 4, ((8, SIDE)[side],), 16, finish)
        for half in range(2):
            copy = pltpu.make_async_copy(
                done.at[side, half],
                out.at[:, pl.ds(side * (SIDE - 8), 8), pl.ds(half * 128, 128)],
                sem.at[side, half],
            )
            copy.start()
            outs.append(copy)
    for copy in outs:
        copy.wait()


VMEM = pl.BlockSpec(memory_space=pltpu.VMEM)
HBM = pl.BlockSpec(memory_space=pltpu.HBM)
DMA = pltpu.SemaphoreType.DMA
FIELD = pltpu.VMEM((2, ROWS, COLS, 128), F32)
COEF = pltpu.VMEM((3, ROWS, COLS, 128), F32)
TURNED = pltpu.VMEM((TURNED_ROWS, 128), F32)
FACTORS = pltpu.VMEM((4, TURNED_ROWS, 128), F32)


def call(kernel, in_specs, out_shape, out_specs, scratch, cost, grant, aliases=None):
    return pl.pallas_call(
        kernel,
        in_specs=in_specs,
        out_shape=out_shape,
        out_specs=out_specs,
        scratch_shapes=scratch,
        input_output_aliases=aliases or {},
        cost_estimate=pl.CostEstimate(flops=cost, bytes_accessed=1 << 20, transcendentals=0),
        compiler_params=pltpu.CompilerParams(vmem_limit_bytes=grant << 20),
    )


def block(east_class, south_class, cond_table, leakage, pad_mask, load):
    gx, gy = lax.axis_size("gx"), lax.axis_size("gy")

    def shift(values, axis, step):
        count = gx if axis == "gx" else gy
        return lax.ppermute(values, axis, [(i, (i + step) % count) for i in range(count)])

    potential = pltpu.HBM((SIDE, SIDE, 256), F32)
    given = [pltpu.with_memory_space_constraint(a, pltpu.HBM) for a in (cond_table, east_class, south_class, leakage, pad_mask, load)]
    to_right, to_left, to_down, to_up, te, ts, tx = call(
        pack_kernel,
        [HBM] * 6,
        [pltpu.VMEM((GY_MSG, 128), F32)] * 2 + [pltpu.VMEM((GX_MSG, 128), F32)] * 2 + [TURNED] * 3,
        [VMEM] * 7,
        [pltpu.SMEM((8,), F32)]
        + [pltpu.VMEM((SIDE, SIDE), kind) for kind in (jnp.int32, jnp.int32, F32, jnp.int32)]
        + [pltpu.VMEM((2, 2, SIDE, 8, 128), F32), DMA((2, 2)), DMA((2, 2, 4)), DMA((5,))],
        1 << 22,
        4,
    )(*given)
    from_left = shift(to_right, "gy", 1)
    from_right = shift(to_left, "gy", -1)
    from_up = shift(to_down, "gx", 1)
    from_down = shift(to_up, "gx", -1)
    s, x1, coef = call(
        first_kernel, [VMEM] * 3 + [HBM], [FIELD, FIELD, COEF], [VMEM] * 3, [FACTORS, DMA((SIDE // 8, 2))], 1 << 25, 4
    )(te, ts, tx, given[5])
    corner_right, corner_left, te2, ts2, tx2 = call(
        corner_kernel, [VMEM] * 5, [pltpu.VMEM((CORNER_MSG, 128), F32)] * 2 + [TURNED] * 3, [VMEM] * 5, [], 1 << 20, 4
    )(te, ts, tx, from_up, from_down)
    corner_from_left = shift(corner_right, "gy", 1)
    corner_from_right = shift(corner_left, "gy", -1)
    *state, out = call(
        main_kernel,
        [VMEM] * 9,
        [FIELD, FIELD, COEF, FIELD, FIELD, potential],
        [VMEM] * 5 + [HBM],
        [FACTORS, pltpu.VMEM((2, SIDE, SIDE, 128), F32), DMA((4, 2))],
        1 << 25,
        6,
        {6 + i: i for i in range(3)},
    )(te2, ts2, tx2, from_up, from_down, to_up, s, x1, coef)
    *state, out = call(
        sides_kernel,
        [VMEM] * 15 + [HBM],
        [FIELD, FIELD, COEF, FIELD, FIELD, potential],
        [VMEM] * 5 + [HBM],
        [TURNED] * 3 + [FACTORS, pltpu.VMEM((2, 2, SIDE, 8, 128), F32), DMA((2, 2))],
        1 << 24,
        4,
        {10 + i: i for i in range(6)},
    )(te2, ts2, tx2, from_up, from_down, to_left, from_left, from_right, corner_from_left, corner_from_right, *state, out)
    return out


def solution(mesh):
    in_specs = (P("gx", "gy"), P("gx", "gy"), P(), P("gx", "gy"), P("gx", "gy"), P("gx", "gy", None))
    return jax.shard_map(block, mesh=mesh, in_specs=in_specs, out_specs=P("gx", "gy", None), check_vma=False)
```

```python
import functools

import jax
import jax.numpy as jnp
from jax import lax
from jax.experimental import pallas as pl
from jax.experimental.pallas import tpu as pltpu
from jax.sharding import PartitionSpec as P


PAD_GAIN = 8.0
SPECTRAL_BOUND = 0.995


SIDE = 64
ROWS = SIDE + 8
COLS = SIDE + 16
MAIN_MSG = 8 * SIDE
TINY_MSG = SIDE + 24
FULL_MSG = MAIN_MSG + 24 + 16
TURNED_ROWS = SIDE + 24
F32 = jnp.float32


def weights():
    b2 = SPECTRAL_BOUND * SPECTRAL_BOUND
    first = 1.0 / (1.0 - b2 / 2.0)
    second = 1.0 / (1.0 - b2 * first / 4.0)
    third = 1.0 / (1.0 - b2 * second / 4.0)
    return first, second, third


W1, W2, W3 = weights()
MIX = W3 + (1.0 - W3) * W1
TOP = W1 * W2 * W3


EAST, SOUTH, ROOT = range(3)


def lanes_of(shape):
    return lax.broadcasted_iota(jnp.int32, shape, 1)


def turn_factors(te, ts, tx, factors, roots, easts, souths):
    for k in roots:
        south = ts[k : k + 8, :]
        ground = tx[k : k + 8, :]
        diagonal = te[k : k + 8, :] + te[k - 1 : k + 7, :] + south + pltpu.roll(south, 1, 1) + ground
        root = 1.0 / jnp.sqrt(diagonal)
        factors[ROOT, k : k + 8, :] = jnp.where(ground > 4.0, -root, root)
    for k in easts:
        factors[EAST, k : k + 8, :] = te[k : k + 8, :] * jnp.abs(factors[ROOT, k : k + 8, :] * factors[ROOT, k + 1 : k + 9, :])
    for k in souths:
        root = jnp.abs(factors[ROOT, k : k + 8, :])
        factors[SOUTH, k : k + 8, :] = ts[k : k + 8, :] * root * pltpu.roll(root, 127, 1)


def spread(values, lane):
    return jnp.broadcast_to(values[:, lane : lane + 1], (8, 128))


def set_factors(coef, row, places, factors, lane):
    for which, c in places:
        value = spread(factors[which, c : c + 8, :], lane)
        coef[which, row, c : c + 8, :] = jnp.abs(value) if which == ROOT else value
    return value


def to_source(s, row, c, signed):
    root = jnp.abs(signed)
    supply = jnp.where(signed < 0.0, PAD_GAIN, 0.0)
    for half in range(2):
        s[half, row, pl.ds(c, 8), :] = (supply - s[half, row, pl.ds(c, 8), :]) * root


def all_at(c):
    return [(EAST, c), (SOUTH, c), (ROOT, c)]


def neighbours(src, coef, base, count, c, emit):
    above = [src[half, base - 1, pl.ds(c, 8), :] for half in range(2)]
    here = [src[half, base, pl.ds(c, 8), :] for half in range(2)]
    north = coef[SOUTH, base - 1, pl.ds(c, 8), :]
    for step in range(count):
        row = base + step
        east = coef[EAST, row, pl.ds(c, 8), :]
        west = coef[EAST, row, pl.ds(c - 1, 8), :]
        south = coef[SOUTH, row, pl.ds(c, 8), :]
        for half in range(2):
            below = src[half, row + 1, pl.ds(c, 8), :]
            total = east * src[half, row, pl.ds(c + 1, 8), :] + west * src[half, row, pl.ds(c - 1, 8), :]
            total = total + (south * below + north * above[half])
            emit(half, row, c, total, here[half])
            above[half], here[half] = here[half], below
        north = south


def sweep(src, coef, first, last, columns, unroll, emit):
    full = (last - first) // unroll
    for c in columns:
        if full == 1:
            neighbours(src, coef, first, unroll, c, emit)
        elif full > 1:

            def trip(index, carry, c=c):
                neighbours(src, coef, first + index * unroll, unroll, c, emit)
                return carry

            lax.fori_loop(0, full, trip, 0)
        if first + full * unroll < last:
            neighbours(src, coef, first + full * unroll, last - first - full * unroll, c, emit)


def adding(target):
    def emit(half, row, c, total, here):
        target[half, row, pl.ds(c, 8), :] = here + total

    return emit


def placing(target):
    def emit(half, row, c, total, here):
        target[half, row, pl.ds(c, 8), :] = total

    return emit


def result(s, u, coef, half, row, c, total):
    value = s[half, row, pl.ds(c, 8), :] + (MIX * u[half, row, pl.ds(c, 8), :] + TOP * total)
    return value * coef[ROOT, row, pl.ds(c, 8), :]


def corner_cells():
    for half in range(2):
        for side in range(2):
            for distance in (1, 2, 3):
                yield (half * 2 + side) * 6 + (0, 3, 5)[distance - 1], half, side, distance


def pack_kernel(*refs):
    small, load = refs[:5], refs[5]
    to_right, to_left, to_down, to_up, tiny_down, tiny_up, te, ts, tx = refs[6:15]
    edge, sem_edge, sem_rows, sem_small = refs[20:]
    table, east_class, south_class, leakage, pad_mask = refs[15:20]
    edges, tops = [], []
    nodes = [pltpu.make_async_copy(source, target, sem_small.at[i]) for i, (source, target) in enumerate(zip(small, refs[15:20]))]
    for copy in nodes:
        copy.start()
    for side in range(2):
        for half in range(2):
            copy = pltpu.make_async_copy(
                load.at[:, pl.ds(side * (SIDE - 8), 8), pl.ds(half * 128, 128)], edge.at[side, half], sem_edge.at[side, half]
            )
            copy.start()
            edges.append(copy)
    for side, message in enumerate((to_up, to_down)):
        for half in range(2):
            for row in range(4):
                copy = pltpu.make_async_copy(
                    load.at[side * (SIDE - 4) + row, :, pl.ds(half * 128, 128)],
                    message.at[pl.ds((half * 4 + row) * SIDE, SIDE), :],
                    sem_rows.at[side, half, row],
                )
                copy.start()
                tops.append(copy)

    for copy in nodes:
        copy.wait()

    def look_up(classes):
        found = jnp.zeros((SIDE, SIDE), F32)
        for label in range(8):
            found = jnp.where(classes == label, table[label], found)
        return found

    zeros = jnp.zeros((SIDE, 128 - SIDE), F32)

    def turned(values):
        return pltpu.roll(jnp.concatenate([values.T, zeros], axis=1), 8, 1)

    east = turned(look_up(east_class[...]))
    south = turned(look_up(south_class[...]))
    ground = turned(leakage[...] + PAD_GAIN * pad_mask[...].astype(F32))
    for target, values in ((te, east), (ts, south), (tx, ground)):
        target[0:8, :] = jnp.zeros((8, 128), F32)
        target[8 : SIDE + 8, :] = values
        target[SIDE + 8 :, :] = jnp.zeros((16, 128), F32)
    lane = lanes_of((SIDE, 128))

    def banded(shifts):
        first, second, third = [
            values if shift == 0 else pltpu.roll(values, shift, 1) for values, shift in zip((east, south, ground), shifts)
        ]
        return jnp.where(lane < 8, first, jnp.where(lane < 16, second, third))

    tiny_down[0:SIDE, :] = banded((64, 72, 80))
    tiny_up[0:SIDE, :] = banded((120, 0, 8))
    for copy in edges:
        copy.wait()
    for offset, half, side, distance in corner_cells():
        count = 4 - distance
        at = SIDE + offset
        columns = slice(8 - count, 8) if side else slice(0, count)
        tiny_down[at : at + count, :] = edge[side, half, SIDE - distance, columns, :]
        tiny_up[at : at + count, :] = edge[side, half, distance - 1, columns, :]
    for side, message in enumerate((to_left, to_right)):
        for half in range(2):
            for row in range(SIDE):
                base = (half * SIDE + row) * 4
                message[base : base + 4, :] = edge[side, half, row, side * 4 : side * 4 + 4, :]
    for copy in tops:
        copy.wait()


def put_conductances(message, base, te, ts, tx, first_east, first_other):
    message[base : base + 5, :] = te[first_east : first_east + 5, :]
    message[base + 5 : base + 9, :] = ts[first_other : first_other + 4, :]
    message[base + 9 : base + 13, :] = tx[first_other : first_other + 4, :]
    message[base + 13 : base + 16, :] = jnp.zeros((3, 128), F32)


def first_kernel(te, ts, tx, load, s, x1, coef, factors, sem):
    def part(group, half):
        return pltpu.make_async_copy(
            load.at[pl.ds(group * 8, 8), :, pl.ds(half * 128, 128)],
            s.at[half, pl.ds(4 + group * 8, 8), pl.ds(8, SIDE), :],
            sem.at[group, half],
        )

    for group in range(SIDE // 8):
        for half in range(2):
            part(group, half).start()
    own = range(8, SIDE + 8, 8)
    turn_factors(te, ts, tx, factors, own, own, own)

    def body(group, carry):
        for half in range(2):
            part(group, half).wait()
        for step in range(8):
            row = group * 8 + 4 + step
            for c in own:
                to_source(s, row, c, set_factors(coef, row, all_at(c), factors, 8 + step))
        for c in own:
            neighbours(s, coef, group * 8 + 3, 8, c, adding(x1))
            for which in range(3):
                factors[which, c : c + 8, :] = pltpu.roll(factors[which, c : c + 8, :], 120, 1)
        return carry

    lax.fori_loop(0, SIDE // 8, body, 0)


def corner_kernel(te, ts, tx, from_up, from_down, right, left, to_right, to_left, te2, ts2, tx2):
    lane = lanes_of((SIDE, 128))
    upper, lower = from_up[0:SIDE, :], from_down[0:SIDE, :]
    for source, target, down, up in ((te, te2, 0, 72), (ts, ts2, 120, 64), (tx, tx2, 112, 56)):
        head = pltpu.roll(upper, down, 1) if down else upper
        tail = pltpu.roll(lower, up, 1)
        own = source[8 : SIDE + 8, :]
        target[0:8, :] = jnp.zeros((8, 128), F32)
        target[8 : SIDE + 8, :] = jnp.where(lane < 8, head, jnp.where(lane < SIDE + 8, own, tail))
        target[SIDE + 8 :, :] = jnp.zeros((16, 128), F32)
    to_right[0:MAIN_MSG, :] = right[...]
    to_left[0:MAIN_MSG, :] = left[...]
    for offset, half, below, distance in corner_cells():
        count = 4 - distance
        origin = from_down if below else from_up
        for side, message in enumerate((to_left, to_right)):
            at = SIDE + (half * 2 + side) * 6 + (0, 3, 5)[distance - 1]
            message[MAIN_MSG + offset : MAIN_MSG + offset + count, :] = origin[at : at + count, :]
    put_conductances(to_right, MAIN_MSG + 24, te2, ts2, tx2, SIDE + 3, SIDE + 4)
    put_conductances(to_left, MAIN_MSG + 24, te2, ts2, tx2, 8, 8)


def main_kernel(te, ts, tx, from_up, from_down, own_up, *rest):
    s, x1, coef, u, t, done, factors = rest[3:]
    own = range(8, SIDE + 8, 8)
    turn_factors(te, ts, tx, factors, own, own, own)
    for half in range(2):
        for row in range(4):
            at = (half * 4 + row) * SIDE
            s[half, row, 8 : SIDE + 8, :] = from_up[at : at + SIDE, :]
            s[half, SIDE + 4 + row, 8 : SIDE + 8, :] = from_down[at : at + SIDE, :]
        s[half, 4, 8 : SIDE + 8, :] = own_up[half * 4 * SIDE : half * 4 * SIDE + SIDE, :]
    for row in (0, 1, 2, 3, 4, SIDE + 3, SIDE + 4, SIDE + 5, SIDE + 6, SIDE + 7):
        for c in own:
            signed = set_factors(coef, row, all_at(c), factors, row + 4)
            if row != SIDE + 3:
                to_source(s, row, c, signed)
    sweep(s, coef, 1, 6, own, 5, adding(x1))
    sweep(s, coef, SIDE + 3, SIDE + 7, own, 4, adding(x1))
    sweep(x1, coef, 2, SIDE + 6, own, 17, placing(u))
    sweep(u, coef, 3, SIDE + 5, own, 22, placing(t))

    def finish(half, row, c, total, here):
        done[half, row - 4, c - 8 : c, :] = result(s, u, coef, half, row, c, total)

    sweep(t, coef, 4, SIDE + 4, range(16, SIDE, 8), 16, finish)


def side_kernel(side, *refs):
    te2, ts2, tx2, message = refs[:4]
    s, x1, coef, u, t, out, done, te, ts, tx, factors, sem = refs[-12:]
    ready = refs[4 if side else 7]
    first, width = (8, SIDE - 16) if side else (SIDE - 8, 8)
    outs = []
    for half in range(2):
        copy = pltpu.make_async_copy(
            ready.at[half, :, pl.ds(8, width), :] if side else ready.at[half],
            out.at[:, pl.ds(first, width), pl.ds(half * 128, 128)],
            sem.at[2, half],
        )
        copy.start()
        outs.append(copy)
    for source, target in ((te2, te), (ts2, ts), (tx2, tx)):
        target[...] = source[...]
    at = MAIN_MSG + 24
    first_east, first_other = (SIDE + 8, SIDE + 8) if side else (3, 4)
    te[first_east : first_east + 5, :] = message[at : at + 5, :]
    ts[first_other : first_other + 4, :] = message[at + 5 : at + 9, :]
    tx[first_other : first_other + 4, :] = message[at + 9 : at + 13, :]
    c = SIDE + 8 if side else 1
    places = [(EAST, SIDE + 7 if side else 1), (SOUTH, c), (ROOT, c)]
    turn_factors(te, ts, tx, factors, (SIDE, c) if side else (c, 8), (places[0][1],), (c,))
    halo = SIDE + 8 if side else 4
    for row in range(SIDE):
        for half in range(2):
            at = (half * SIDE + row) * 4
            s[half, row + 4, halo : halo + 4, :] = message[at : at + 4, :]
            if side == 0:
                s[half, row + 4, 8:9, :] = refs[4][at : at + 1, :]
    if side == 0:
        for half in range(2):
            for row in range(4):
                at = (half * 4 + row) * SIDE
                s[half, row, 8:9, :] = refs[5][at : at + 1, :]
                s[half, SIDE + 4 + row, 8:9, :] = refs[6][at : at + 1, :]
    for offset, half, below, distance in corner_cells():
        count = 4 - distance
        row = SIDE + 3 + distance if below else 4 - distance
        start = SIDE + 8 if side else 8 - count
        s[half, row, start : start + count, :] = message[MAIN_MSG + offset : MAIN_MSG + offset + count, :]

    def body(group, carry):
        for step in range(8):
            row = group * 8 + step
            to_source(s, row, c, set_factors(coef, row, places, factors, 4 + step))
        for which, k in places:
            factors[which, k : k + 8, :] = pltpu.roll(factors[which, k : k + 8, :], 120, 1)
        return carry

    lax.fori_loop(0, ROWS // 8, body, 0)
    sweep(s, coef, 1, SIDE + 7, (SIDE + 4 if side else 4,), 14, adding(x1))
    sweep(x1, coef, 2, SIDE + 6, (SIDE + 3 if side else 5,), 17, placing(u))
    sweep(u, coef, 3, SIDE + 5, (SIDE + 2 if side else 6,), 22, placing(t))

    def finish(half, row, c, total, here):
        done[half, row - 4, :, :] = result(s, u, coef, half, row, c, total)

    for part in range(2):
        rows = pl.ds(part * (SIDE // 2), SIDE // 2)
        sweep(t, coef, 4 + part * (SIDE // 2), 4 + (part + 1) * (SIDE // 2), (SIDE if side else 8,), 16, finish)
        for half in range(2):
            if side == 0:
                copy = pltpu.make_async_copy(
                    done.at[half, rows],
                    out.at[rows, pl.ds(0, 8), pl.ds(half * 128, 128)],
                    sem.at[part, half],
                )
                copy.start()
                outs.append(copy)
    for copy in outs:
        copy.wait()


VMEM = pl.BlockSpec(memory_space=pltpu.VMEM)
HBM = pl.BlockSpec(memory_space=pltpu.HBM)
DMA = pltpu.SemaphoreType.DMA
FIELD = pltpu.VMEM((2, ROWS, COLS, 128), F32)
COEF = pltpu.VMEM((3, ROWS, COLS, 128), F32)
TURNED = pltpu.VMEM((TURNED_ROWS, 128), F32)
FACTORS = pltpu.VMEM((3, TURNED_ROWS, 128), F32)


def call(kernel, in_specs, out_shape, out_specs, scratch, cost, grant, aliases=None):
    return pl.pallas_call(
        kernel,
        in_specs=in_specs,
        out_shape=out_shape,
        out_specs=out_specs,
        scratch_shapes=scratch,
        input_output_aliases=aliases or {},
        cost_estimate=pl.CostEstimate(flops=cost, bytes_accessed=1 << 20, transcendentals=0),
        compiler_params=pltpu.CompilerParams(vmem_limit_bytes=grant << 20),
    )


def block(east_class, south_class, cond_table, leakage, pad_mask, load):
    gx, gy = lax.axis_size("gx"), lax.axis_size("gy")

    def shift(values, axis, step):
        count = gx if axis == "gx" else gy
        return lax.ppermute(values, axis, [(i, (i + step) % count) for i in range(count)])

    potential = pltpu.HBM((SIDE, SIDE, 256), F32)
    given = [pltpu.with_memory_space_constraint(a, pltpu.HBM) for a in (cond_table, east_class, south_class, leakage, pad_mask, load)]
    right, left, to_down, to_up, tiny_down, tiny_up, te, ts, tx = call(
        pack_kernel,
        [HBM] * 6,
        [pltpu.VMEM((MAIN_MSG, 128), F32)] * 4 + [pltpu.VMEM((TINY_MSG, 128), F32)] * 2 + [TURNED] * 3,
        [VMEM] * 9,
        [pltpu.SMEM((8,), F32)]
        + [pltpu.VMEM((SIDE, SIDE), kind) for kind in (jnp.int32, jnp.int32, F32, jnp.int32)]
        + [pltpu.VMEM((2, 2, SIDE, 8, 128), F32), DMA((2, 2)), DMA((2, 2, 4)), DMA((5,))],
        1 << 22,
        4,
    )(*given)
    tiny_from_up = shift(tiny_down, "gx", 1)
    tiny_from_down = shift(tiny_up, "gx", -1)
    from_up = shift(to_down, "gx", 1)
    from_down = shift(to_up, "gx", -1)
    to_right, to_left, te2, ts2, tx2 = call(
        corner_kernel, [VMEM] * 7, [pltpu.VMEM((FULL_MSG, 128), F32)] * 2 + [TURNED] * 3, [VMEM] * 5, [], 1 << 20, 4
    )(te, ts, tx, tiny_from_up, tiny_from_down, right, left)
    from_left = shift(to_right, "gy", 1)
    from_right = shift(to_left, "gy", -1)
    s, x1, coef = call(
        first_kernel, [VMEM] * 3 + [HBM], [FIELD, FIELD, COEF], [VMEM] * 3, [FACTORS, DMA((SIDE // 8, 2))], 1 << 25, 4
    )(te, ts, tx, given[5])
    *state, middle = call(
        main_kernel,
        [VMEM] * 9,
        [FIELD, FIELD, COEF, FIELD, FIELD, pltpu.VMEM((2, SIDE, SIDE, 128), F32)],
        [VMEM] * 6,
        [FACTORS],
        1 << 25,
        4,
        {6 + i: i for i in range(3)},
    )(te2, ts2, tx2, from_up, from_down, to_up, s, x1, coef)
    strip = pltpu.VMEM((2, SIDE, 8, 128), F32)
    *state, out, right_strip = call(
        functools.partial(side_kernel, 1),
        [VMEM] * 10,
        [FIELD, FIELD, COEF, FIELD, FIELD, potential, strip],
        [VMEM] * 5 + [HBM, VMEM],
        [TURNED] * 3 + [FACTORS, DMA((3, 2))],
        1 << 23,
        4,
        {5 + i: i for i in range(5)},
    )(te2, ts2, tx2, from_right, middle, *state)
    *state, out = call(
        functools.partial(side_kernel, 0),
        [VMEM] * 13 + [HBM],
        [FIELD, FIELD, COEF, FIELD, FIELD, potential],
        [VMEM] * 5 + [HBM],
        [strip] + [TURNED] * 3 + [FACTORS, DMA((3, 2))],
        1 << 23,
        4,
        {8 + i: i for i in range(6)},
    )(te2, ts2, tx2, from_left, left, from_up, from_down, right_strip, *state, out)
    return out


def solution(mesh):
    in_specs = (P("gx", "gy"), P("gx", "gy"), P(), P("gx", "gy"), P("gx", "gy"), P("gx", "gy", None))
    return jax.shard_map(block, mesh=mesh, in_specs=in_specs, out_specs=P("gx", "gy", None), check_vma=False)
```

```python
import functools

import jax
import jax.numpy as jnp
from jax import lax
from jax.experimental import pallas as pl
from jax.experimental.pallas import tpu as pltpu
from jax.sharding import PartitionSpec as P


PAD_GAIN = 8.0
SPECTRAL_BOUND = 0.995


SIDE = 64
ROWS = SIDE + 8
COLS = SIDE + 16
MAIN_MSG = 8 * SIDE
TINY_MSG = SIDE + 24
FULL_MSG = MAIN_MSG + 24 + 16
TURNED_ROWS = SIDE + 24
F32 = jnp.float32


def weights():
    b2 = SPECTRAL_BOUND * SPECTRAL_BOUND
    first = 1.0 / (1.0 - b2 / 2.0)
    second = 1.0 / (1.0 - b2 * first / 4.0)
    third = 1.0 / (1.0 - b2 * second / 4.0)
    return first, second, third


W1, W2, W3 = weights()
MIX = W3 + (1.0 - W3) * W1
TOP = W1 * W2 * W3


EAST, SOUTH, ROOT = range(3)


def lanes_of(shape):
    return lax.broadcasted_iota(jnp.int32, shape, 1)


def turn_factors(te, ts, tx, factors, roots, easts, souths):
    for k in roots:
        south = ts[k : k + 8, :]
        ground = tx[k : k + 8, :]
        diagonal = te[k : k + 8, :] + te[k - 1 : k + 7, :] + south + pltpu.roll(south, 1, 1) + ground
        root = 1.0 / jnp.sqrt(diagonal)
        factors[ROOT, k : k + 8, :] = jnp.where(ground > 4.0, -root, root)
    for k in easts:
        factors[EAST, k : k + 8, :] = te[k : k + 8, :] * jnp.abs(factors[ROOT, k : k + 8, :] * factors[ROOT, k + 1 : k + 9, :])
    for k in souths:
        root = jnp.abs(factors[ROOT, k : k + 8, :])
        factors[SOUTH, k : k + 8, :] = ts[k : k + 8, :] * root * pltpu.roll(root, 127, 1)


def spread(values, lane):
    return jnp.broadcast_to(values[:, lane : lane + 1], (8, 128))


def set_factors(coef, row, places, factors, lane):
    for which, c in places:
        value = spread(factors[which, c : c + 8, :], lane)
        coef[which, row, c : c + 8, :] = jnp.abs(value) if which == ROOT else value
    return value


def to_source(s, row, c, signed):
    root = jnp.abs(signed)
    supply = jnp.where(signed < 0.0, PAD_GAIN, 0.0)
    for half in range(2):
        s[half, row, pl.ds(c, 8), :] = (supply - s[half, row, pl.ds(c, 8), :]) * root


def all_at(c):
    return [(EAST, c), (SOUTH, c), (ROOT, c)]


def neighbours(src, coef, base, count, c, emit):
    above = [src[half, base - 1, pl.ds(c, 8), :] for half in range(2)]
    here = [src[half, base, pl.ds(c, 8), :] for half in range(2)]
    north = coef[SOUTH, base - 1, pl.ds(c, 8), :]
    for step in range(count):
        row = base + step
        east = coef[EAST, row, pl.ds(c, 8), :]
        west = coef[EAST, row, pl.ds(c - 1, 8), :]
        south = coef[SOUTH, row, pl.ds(c, 8), :]
        for half in range(2):
            below = src[half, row + 1, pl.ds(c, 8), :]
            total = east * src[half, row, pl.ds(c + 1, 8), :] + west * src[half, row, pl.ds(c - 1, 8), :]
            total = total + (south * below + north * above[half])
            emit(half, row, c, total, here[half])
            above[half], here[half] = here[half], below
        north = south


def sweep(src, coef, first, last, columns, unroll, emit):
    full = (last - first) // unroll
    for c in columns:
        if full == 1:
            neighbours(src, coef, first, unroll, c, emit)
        elif full > 1:

            def trip(index, carry, c=c):
                neighbours(src, coef, first + index * unroll, unroll, c, emit)
                return carry

            lax.fori_loop(0, full, trip, 0)
        if first + full * unroll < last:
            neighbours(src, coef, first + full * unroll, last - first - full * unroll, c, emit)


def adding(target):
    def emit(half, row, c, total, here):
        target[half, row, pl.ds(c, 8), :] = here + total

    return emit


def placing(target):
    def emit(half, row, c, total, here):
        target[half, row, pl.ds(c, 8), :] = total

    return emit


def result(s, u, coef, half, row, c, total):
    value = s[half, row, pl.ds(c, 8), :] + (MIX * u[half, row, pl.ds(c, 8), :] + TOP * total)
    return value * coef[ROOT, row, pl.ds(c, 8), :]


def even_row():
    return lax.rem(lax.axis_index("gx"), 2) == 0


def corner_cells():
    for half in range(2):
        for side in range(2):
            for distance in (1, 2, 3):
                yield (half * 2 + side) * 6 + (0, 3, 5)[distance - 1], half, side, distance


def pack_kernel(*refs):
    small, load = refs[:5], refs[5]
    to_right, to_left, to_near, to_far, tiny_near, tiny_far, te, ts, tx = refs[6:15]
    even = even_row()
    near, far = jnp.where(even, SIDE - 4, 0), jnp.where(even, 0, SIDE - 4)
    edge, sem_edge, sem_rows, sem_small = refs[20:]
    table, east_class, south_class, leakage, pad_mask = refs[15:20]
    edges, tops = [], []
    nodes = [pltpu.make_async_copy(source, target, sem_small.at[i]) for i, (source, target) in enumerate(zip(small, refs[15:20]))]
    for copy in nodes:
        copy.start()
    for side in range(2):
        for half in range(2):
            copy = pltpu.make_async_copy(
                load.at[:, pl.ds(side * (SIDE - 8), 8), pl.ds(half * 128, 128)], edge.at[side, half], sem_edge.at[side, half]
            )
            copy.start()
            edges.append(copy)
    for place, (start, message) in enumerate(((near, to_near), (far, to_far))):
        for half in range(2):
            for row in range(4):
                copy = pltpu.make_async_copy(
                    load.at[start + row, :, pl.ds(half * 128, 128)],
                    message.at[pl.ds((half * 4 + row) * SIDE, SIDE), :],
                    sem_rows.at[place, half, row],
                )
                copy.start()
                tops.append(copy)

    for copy in nodes:
        copy.wait()

    def look_up(classes):
        found = jnp.zeros((SIDE, SIDE), F32)
        for label in range(8):
            found = jnp.where(classes == label, table[label], found)
        return found

    zeros = jnp.zeros((SIDE, 128 - SIDE), F32)

    def turned(values):
        return pltpu.roll(jnp.concatenate([values.T, zeros], axis=1), 8, 1)

    east = turned(look_up(east_class[...]))
    south = turned(look_up(south_class[...]))
    ground = turned(leakage[...] + PAD_GAIN * pad_mask[...].astype(F32))
    for target, values in ((te, east), (ts, south), (tx, ground)):
        target[0:8, :] = jnp.zeros((8, 128), F32)
        target[8 : SIDE + 8, :] = values
        target[SIDE + 8 :, :] = jnp.zeros((16, 128), F32)
    lane = lanes_of((SIDE, 128))

    def banded(shifts):
        first, second, third = [
            values if shift == 0 else pltpu.roll(values, shift, 1) for values, shift in zip((east, south, ground), shifts)
        ]
        return jnp.where(lane < 8, first, jnp.where(lane < 16, second, third))

    lower, upper = banded((64, 72, 80)), banded((120, 0, 8))
    tiny_near[0:SIDE, :] = jnp.where(even, lower, upper)
    tiny_far[0:SIDE, :] = jnp.where(even, upper, lower)
    for copy in edges:
        copy.wait()
    for offset, half, side, distance in corner_cells():
        count = 4 - distance
        at = SIDE + offset
        columns = slice(8 - count, 8) if side else slice(0, count)
        tiny_near[at : at + count, :] = edge[side, half, jnp.where(even, SIDE - distance, distance - 1), columns, :]
        tiny_far[at : at + count, :] = edge[side, half, jnp.where(even, distance - 1, SIDE - distance), columns, :]
    for side, message in enumerate((to_left, to_right)):
        for half in range(2):
            for row in range(SIDE):
                base = (half * SIDE + row) * 4
                message[base : base + 4, :] = edge[side, half, row, side * 4 : side * 4 + 4, :]
    for copy in tops:
        copy.wait()


def put_conductances(message, base, te, ts, tx, first_east, first_other):
    message[base : base + 5, :] = te[first_east : first_east + 5, :]
    message[base + 5 : base + 9, :] = ts[first_other : first_other + 4, :]
    message[base + 9 : base + 13, :] = tx[first_other : first_other + 4, :]
    message[base + 13 : base + 16, :] = jnp.zeros((3, 128), F32)


def first_kernel(te, ts, tx, load, s, x1, coef, factors, sem):
    def part(group, half):
        return pltpu.make_async_copy(
            load.at[pl.ds(group * 8, 8), :, pl.ds(half * 128, 128)],
            s.at[half, pl.ds(4 + group * 8, 8), pl.ds(8, SIDE), :],
            sem.at[group, half],
        )

    for group in range(SIDE // 8):
        for half in range(2):
            part(group, half).start()
    own = range(8, SIDE + 8, 8)
    turn_factors(te, ts, tx, factors, own, own, own)

    def body(group, carry):
        for half in range(2):
            part(group, half).wait()
        for step in range(8):
            row = group * 8 + 4 + step
            for c in own:
                to_source(s, row, c, set_factors(coef, row, all_at(c), factors, 8 + step))
        for c in own:
            neighbours(s, coef, group * 8 + 3, 8, c, adding(x1))
            for which in range(3):
                factors[which, c : c + 8, :] = pltpu.roll(factors[which, c : c + 8, :], 120, 1)
        return carry

    lax.fori_loop(0, SIDE // 8, body, 0)


def corner_kernel(te, ts, tx, near, far, right, left, to_right, to_left, te2, ts2, tx2):
    lane = lanes_of((SIDE, 128))
    even = even_row()
    upper = jnp.where(even, far[0:SIDE, :], near[0:SIDE, :])
    lower = jnp.where(even, near[0:SIDE, :], far[0:SIDE, :])
    for source, target, down, up in ((te, te2, 0, 72), (ts, ts2, 120, 64), (tx, tx2, 112, 56)):
        head = pltpu.roll(upper, down, 1) if down else upper
        tail = pltpu.roll(lower, up, 1)
        own = source[8 : SIDE + 8, :]
        target[0:8, :] = jnp.zeros((8, 128), F32)
        target[8 : SIDE + 8, :] = jnp.where(lane < 8, head, jnp.where(lane < SIDE + 8, own, tail))
        target[SIDE + 8 :, :] = jnp.zeros((16, 128), F32)
    to_right[0:MAIN_MSG, :] = right[...]
    to_left[0:MAIN_MSG, :] = left[...]
    for offset, half, below, distance in corner_cells():
        count = 4 - distance
        for side, message in enumerate((to_left, to_right)):
            at = SIDE + (half * 2 + side) * 6 + (0, 3, 5)[distance - 1]
            first, second = (near, far) if below else (far, near)
            message[MAIN_MSG + offset : MAIN_MSG + offset + count, :] = jnp.where(
                even, first[at : at + count, :], second[at : at + count, :]
            )
    put_conductances(to_right, MAIN_MSG + 24, te2, ts2, tx2, SIDE + 3, SIDE + 4)
    put_conductances(to_left, MAIN_MSG + 24, te2, ts2, tx2, 8, 8)


def main_kernel(te, ts, tx, near, far, own_near, own_far, *rest):
    s, x1, coef, u, t, out, factors, done, sem = rest[3:]
    even = even_row()
    own = range(8, SIDE + 8, 8)
    turn_factors(te, ts, tx, factors, own, own, own)
    for half in range(2):
        for row in range(4):
            at = (half * 4 + row) * SIDE
            one, other = near[at : at + SIDE, :], far[at : at + SIDE, :]
            s[half, row, 8 : SIDE + 8, :] = jnp.where(even, other, one)
            s[half, SIDE + 4 + row, 8 : SIDE + 8, :] = jnp.where(even, one, other)
        at = half * 4 * SIDE
        s[half, 4, 8 : SIDE + 8, :] = jnp.where(even, own_far[at : at + SIDE, :], own_near[at : at + SIDE, :])
    for row in (0, 1, 2, 3, 4, SIDE + 3, SIDE + 4, SIDE + 5, SIDE + 6, SIDE + 7):
        for c in own:
            signed = set_factors(coef, row, all_at(c), factors, row + 4)
            if row != SIDE + 3:
                to_source(s, row, c, signed)
    sweep(s, coef, 1, 6, own, 5, adding(x1))
    sweep(s, coef, SIDE + 3, SIDE + 7, own, 4, adding(x1))
    sweep(x1, coef, 2, SIDE + 6, own, 17, placing(u))
    sweep(u, coef, 3, SIDE + 5, own, 22, placing(t))

    def finish(half, row, c, total, here):
        done[half, row - 4, c - 8 : c, :] = result(s, u, coef, half, row, c, total)

    outs = []
    for part in range(4):
        rows = pl.ds(part * 16, 16)
        sweep(t, coef, 4 + part * 16, 20 + part * 16, range(16, SIDE, 8), 16, finish)
        for half in range(2):
            copy = pltpu.make_async_copy(
                done.at[half, rows, pl.ds(8, SIDE - 16), :],
                out.at[rows, pl.ds(8, SIDE - 16), pl.ds(half * 128, 128)],
                sem.at[part, half],
            )
            copy.start()
            outs.append(copy)
    for copy in outs:
        copy.wait()


def side_kernel(side, *refs):
    te2, ts2, tx2, message = refs[:4]
    if side:
        s, x1, coef, u, t, out, done, te, ts, tx, factors, sem = refs[-12:]
    else:
        s, x1, coef, u, t, done, te, ts, tx, factors = refs[-10:]
    outs = []
    if side:
        for half in range(2):
            copy = pltpu.make_async_copy(
                refs[4].at[half], out.at[:, pl.ds(0, 8), pl.ds(half * 128, 128)], sem.at[2, half]
            )
            copy.start()
            outs.append(copy)
    for source, target in ((te2, te), (ts2, ts), (tx2, tx)):
        target[...] = source[...]
    at = MAIN_MSG + 24
    first_east, first_other = (SIDE + 8, SIDE + 8) if side else (3, 4)
    te[first_east : first_east + 5, :] = message[at : at + 5, :]
    ts[first_other : first_other + 4, :] = message[at + 5 : at + 9, :]
    tx[first_other : first_other + 4, :] = message[at + 9 : at + 13, :]
    c = SIDE + 8 if side else 1
    places = [(EAST, SIDE + 7 if side else 1), (SOUTH, c), (ROOT, c)]
    turn_factors(te, ts, tx, factors, (SIDE, c) if side else (c, 8), (places[0][1],), (c,))
    halo = SIDE + 8 if side else 4
    for row in range(SIDE):
        for half in range(2):
            at = (half * SIDE + row) * 4
            s[half, row + 4, halo : halo + 4, :] = message[at : at + 4, :]
            if side == 0:
                s[half, row + 4, 8:9, :] = refs[4][at : at + 1, :]
    if side == 0:
        even = even_row()
        for half in range(2):
            for row in range(4):
                at = (half * 4 + row) * SIDE
                one, other = refs[5][at : at + 1, :], refs[6][at : at + 1, :]
                s[half, row, 8:9, :] = jnp.where(even, other, one)
                s[half, SIDE + 4 + row, 8:9, :] = jnp.where(even, one, other)
    for offset, half, below, distance in corner_cells():
        count = 4 - distance
        row = SIDE + 3 + distance if below else 4 - distance
        start = SIDE + 8 if side else 8 - count
        s[half, row, start : start + count, :] = message[MAIN_MSG + offset : MAIN_MSG + offset + count, :]

    def body(group, carry):
        for step in range(8):
            row = group * 8 + step
            to_source(s, row, c, set_factors(coef, row, places, factors, 4 + step))
        for which, k in places:
            factors[which, k : k + 8, :] = pltpu.roll(factors[which, k : k + 8, :], 120, 1)
        return carry

    lax.fori_loop(0, ROWS // 8, body, 0)
    sweep(s, coef, 1, SIDE + 7, (SIDE + 4 if side else 4,), 14, adding(x1))
    sweep(x1, coef, 2, SIDE + 6, (SIDE + 3 if side else 5,), 17, placing(u))
    sweep(u, coef, 3, SIDE + 5, (SIDE + 2 if side else 6,), 22, placing(t))

    def finish(half, row, c, total, here):
        done[half, row - 4, :, :] = result(s, u, coef, half, row, c, total)

    for part in range(2):
        rows = pl.ds(part * (SIDE // 2), SIDE // 2)
        sweep(t, coef, 4 + part * (SIDE // 2), 4 + (part + 1) * (SIDE // 2), (SIDE if side else 8,), 16, finish)
        for half in range(2):
            if side:
                copy = pltpu.make_async_copy(
                    done.at[half, rows],
                    out.at[rows, pl.ds(SIDE - 8, 8), pl.ds(half * 128, 128)],
                    sem.at[part, half],
                )
                copy.start()
                outs.append(copy)
    for copy in outs:
        copy.wait()


VMEM = pl.BlockSpec(memory_space=pltpu.VMEM)
HBM = pl.BlockSpec(memory_space=pltpu.HBM)
DMA = pltpu.SemaphoreType.DMA
FIELD = pltpu.VMEM((2, ROWS, COLS, 128), F32)
COEF = pltpu.VMEM((3, ROWS, COLS, 128), F32)
TURNED = pltpu.VMEM((TURNED_ROWS, 128), F32)
FACTORS = pltpu.VMEM((3, TURNED_ROWS, 128), F32)


def call(kernel, in_specs, out_shape, out_specs, scratch, cost, grant, aliases=None):
    return pl.pallas_call(
        kernel,
        in_specs=in_specs,
        out_shape=out_shape,
        out_specs=out_specs,
        scratch_shapes=scratch,
        input_output_aliases=aliases or {},
        cost_estimate=pl.CostEstimate(flops=cost, bytes_accessed=1 << 20, transcendentals=0),
        compiler_params=pltpu.CompilerParams(vmem_limit_bytes=grant << 20),
    )


def exchange(near, far):
    count = lax.axis_size("gx")
    near = lax.ppermute(near, "gx", [(i, i ^ 1) for i in range(count)])
    far = lax.ppermute(far, "gx", [(i, (i - 1 + 2 * (i % 2)) % count) for i in range(count)])
    return near, far


def block(east_class, south_class, cond_table, leakage, pad_mask, load):
    def shift(values, step):
        count = lax.axis_size("gy")
        return lax.ppermute(values, "gy", [(i, (i + step) % count) for i in range(count)])

    potential = pltpu.HBM((SIDE, SIDE, 256), F32)
    given = [pltpu.with_memory_space_constraint(a, pltpu.HBM) for a in (cond_table, east_class, south_class, leakage, pad_mask, load)]
    right, left, to_near, to_far, tiny_near, tiny_far, te, ts, tx = call(
        pack_kernel,
        [HBM] * 6,
        [pltpu.VMEM((MAIN_MSG, 128), F32)] * 4 + [pltpu.VMEM((TINY_MSG, 128), F32)] * 2 + [TURNED] * 3,
        [VMEM] * 9,
        [pltpu.SMEM((8,), F32)]
        + [pltpu.VMEM((SIDE, SIDE), kind) for kind in (jnp.int32, jnp.int32, F32, jnp.int32)]
        + [pltpu.VMEM((2, 2, SIDE, 8, 128), F32), DMA((2, 2)), DMA((2, 2, 4)), DMA((5,))],
        1 << 22,
        4,
    )(*given)
    tiny_one, tiny_other = exchange(tiny_near, tiny_far)
    one, other = exchange(to_near, to_far)
    to_right, to_left, te2, ts2, tx2 = call(
        corner_kernel, [VMEM] * 7, [pltpu.VMEM((FULL_MSG, 128), F32)] * 2 + [TURNED] * 3, [VMEM] * 5, [], 1 << 20, 4
    )(te, ts, tx, tiny_one, tiny_other, right, left)
    from_left = shift(to_right, 1)
    from_right = shift(to_left, -1)
    s, x1, coef = call(
        first_kernel, [VMEM] * 3 + [HBM], [FIELD, FIELD, COEF], [VMEM] * 3, [FACTORS, DMA((SIDE // 8, 2))], 1 << 25, 4
    )(te, ts, tx, given[5])
    *state, out = call(
        main_kernel,
        [VMEM] * 10,
        [FIELD, FIELD, COEF, FIELD, FIELD, potential],
        [VMEM] * 5 + [HBM],
        [FACTORS, pltpu.VMEM((2, SIDE, SIDE, 128), F32), DMA((4, 2))],
        1 << 25,
        6,
        {7 + i: i for i in range(3)},
    )(te2, ts2, tx2, one, other, to_near, to_far, s, x1, coef)
    strip = pltpu.VMEM((2, SIDE, 8, 128), F32)
    *state, left_strip = call(
        functools.partial(side_kernel, 0),
        [VMEM] * 12,
        [FIELD, FIELD, COEF, FIELD, FIELD, strip],
        [VMEM] * 6,
        [TURNED] * 3 + [FACTORS],
        1 << 23,
        4,
        {7 + i: i for i in range(5)},
    )(te2, ts2, tx2, from_left, left, one, other, *state)
    *state, out = call(
        functools.partial(side_kernel, 1),
        [VMEM] * 10 + [HBM],
        [FIELD, FIELD, COEF, FIELD, FIELD, potential],
        [VMEM] * 5 + [HBM],
        [strip] + [TURNED] * 3 + [FACTORS, DMA((3, 2))],
        1 << 23,
        4,
        {5 + i: i for i in range(6)},
    )(te2, ts2, tx2, from_right, left_strip, *state, out)
    return out


def solution(mesh):
    in_specs = (P("gx", "gy"), P("gx", "gy"), P(), P("gx", "gy"), P("gx", "gy"), P("gx", "gy", None))
    return jax.shard_map(block, mesh=mesh, in_specs=in_specs, out_specs=P("gx", "gy", None), check_vma=False)
```

```python
import functools

import jax
import jax.numpy as jnp
from jax import lax
from jax.experimental import pallas as pl
from jax.experimental.pallas import tpu as pltpu
from jax.sharding import PartitionSpec as P


PAD_GAIN = 8.0
SPECTRAL_BOUND = 0.995


SIDE = 64
ROWS = SIDE + 8
COLS = SIDE + 16
MAIN_MSG = 8 * SIDE
TINY_MSG = SIDE + 24
FULL_MSG = MAIN_MSG + 24 + 16
TURNED_ROWS = SIDE + 24
F32 = jnp.float32


def weights():
    b2 = SPECTRAL_BOUND * SPECTRAL_BOUND
    first = 1.0 / (1.0 - b2 / 2.0)
    second = 1.0 / (1.0 - b2 * first / 4.0)
    third = 1.0 / (1.0 - b2 * second / 4.0)
    return first, second, third


W1, W2, W3 = weights()
MIX = W3 + (1.0 - W3) * W1
TOP = W1 * W2 * W3


EAST, SOUTH, ROOT = range(3)


def lanes_of(shape):
    return lax.broadcasted_iota(jnp.int32, shape, 1)


def turn_factors(te, ts, tx, factors, roots, easts, souths):
    for k in roots:
        south = ts[k : k + 8, :]
        ground = tx[k : k + 8, :]
        diagonal = te[k : k + 8, :] + te[k - 1 : k + 7, :] + south + pltpu.roll(south, 1, 1) + ground
        root = 1.0 / jnp.sqrt(diagonal)
        factors[ROOT, k : k + 8, :] = jnp.where(ground > 4.0, -root, root)
    for k in easts:
        factors[EAST, k : k + 8, :] = te[k : k + 8, :] * jnp.abs(factors[ROOT, k : k + 8, :] * factors[ROOT, k + 1 : k + 9, :])
    for k in souths:
        root = jnp.abs(factors[ROOT, k : k + 8, :])
        factors[SOUTH, k : k + 8, :] = ts[k : k + 8, :] * root * pltpu.roll(root, 127, 1)


def spread(values, lane):
    return jnp.broadcast_to(values[:, lane : lane + 1], (8, 128))


def set_factors(coef, row, places, factors, lane):
    for which, c in places:
        value = spread(factors[which, c : c + 8, :], lane)
        coef[which, row, c : c + 8, :] = jnp.abs(value) if which == ROOT else value
    return value


def to_source(s, row, c, signed):
    root = jnp.abs(signed)
    supply = jnp.where(signed < 0.0, PAD_GAIN, 0.0)
    for half in range(2):
        s[half, row, pl.ds(c, 8), :] = (supply - s[half, row, pl.ds(c, 8), :]) * root


def all_at(c):
    return [(EAST, c), (SOUTH, c), (ROOT, c)]


def neighbours(src, coef, base, count, c, emit):
    above = [src[half, base - 1, pl.ds(c, 8), :] for half in range(2)]
    here = [src[half, base, pl.ds(c, 8), :] for half in range(2)]
    north = coef[SOUTH, base - 1, pl.ds(c, 8), :]
    for step in range(count):
        row = base + step
        east = coef[EAST, row, pl.ds(c, 8), :]
        west = coef[EAST, row, pl.ds(c - 1, 8), :]
        south = coef[SOUTH, row, pl.ds(c, 8), :]
        for half in range(2):
            below = src[half, row + 1, pl.ds(c, 8), :]
            total = east * src[half, row, pl.ds(c + 1, 8), :] + west * src[half, row, pl.ds(c - 1, 8), :]
            total = total + (south * below + north * above[half])
            emit(half, row, c, total, here[half])
            above[half], here[half] = here[half], below
        north = south


def sweep(src, coef, first, last, columns, unroll, emit):
    full = (last - first) // unroll
    for c in columns:
        if full == 1:
            neighbours(src, coef, first, unroll, c, emit)
        elif full > 1:

            def trip(index, carry, c=c):
                neighbours(src, coef, first + index * unroll, unroll, c, emit)
                return carry

            lax.fori_loop(0, full, trip, 0)
        if first + full * unroll < last:
            neighbours(src, coef, first + full * unroll, last - first - full * unroll, c, emit)


def adding(target):
    def emit(half, row, c, total, here):
        target[half, row, pl.ds(c, 8), :] = here + total

    return emit


def placing(target):
    def emit(half, row, c, total, here):
        target[half, row, pl.ds(c, 8), :] = total

    return emit


def result(s, u, coef, half, row, c, total):
    value = s[half, row, pl.ds(c, 8), :] + (MIX * u[half, row, pl.ds(c, 8), :] + TOP * total)
    return value * coef[ROOT, row, pl.ds(c, 8), :]


def even_row():
    return lax.rem(lax.axis_index("gx"), 2) == 0


def corner_cells():
    for half in range(2):
        for side in range(2):
            for distance in (1, 2, 3):
                yield (half * 2 + side) * 6 + (0, 3, 5)[distance - 1], half, side, distance


def pack_kernel(*refs):
    small, load = refs[:5], refs[5]
    to_right, to_left, to_near, to_far, tiny_near, tiny_far, te, ts, tx = refs[6:15]
    even = even_row()
    near, far = jnp.where(even, SIDE - 4, 0), jnp.where(even, 0, SIDE - 4)
    edge, sem_edge, sem_rows, sem_small = refs[20:]
    table, east_class, south_class, leakage, pad_mask = refs[15:20]
    edges, tops = [], []
    nodes = [pltpu.make_async_copy(source, target, sem_small.at[i]) for i, (source, target) in enumerate(zip(small, refs[15:20]))]
    for copy in nodes:
        copy.start()
    for side in range(2):
        for half in range(2):
            copy = pltpu.make_async_copy(
                load.at[:, pl.ds(side * (SIDE - 8), 8), pl.ds(half * 128, 128)], edge.at[side, half], sem_edge.at[side, half]
            )
            copy.start()
            edges.append(copy)
    for place, (start, message) in enumerate(((near, to_near), (far, to_far))):
        for half in range(2):
            for row in range(4):
                copy = pltpu.make_async_copy(
                    load.at[start + row, :, pl.ds(half * 128, 128)],
                    message.at[pl.ds((half * 4 + row) * SIDE, SIDE), :],
                    sem_rows.at[place, half, row],
                )
                copy.start()
                tops.append(copy)

    for copy in nodes:
        copy.wait()

    def look_up(classes):
        found = jnp.zeros((SIDE, SIDE), F32)
        for label in range(8):
            found = jnp.where(classes == label, table[label], found)
        return found

    zeros = jnp.zeros((SIDE, 128 - SIDE), F32)

    def turned(values):
        return pltpu.roll(jnp.concatenate([values.T, zeros], axis=1), 8, 1)

    east = turned(look_up(east_class[...]))
    south = turned(look_up(south_class[...]))
    ground = turned(leakage[...] + PAD_GAIN * pad_mask[...].astype(F32))
    for target, values in ((te, east), (ts, south), (tx, ground)):
        target[0:8, :] = jnp.zeros((8, 128), F32)
        target[8 : SIDE + 8, :] = values
        target[SIDE + 8 :, :] = jnp.zeros((16, 128), F32)
    lane = lanes_of((SIDE, 128))

    def banded(shifts):
        first, second, third = [
            values if shift == 0 else pltpu.roll(values, shift, 1) for values, shift in zip((east, south, ground), shifts)
        ]
        return jnp.where(lane < 8, first, jnp.where(lane < 16, second, third))

    lower, upper = banded((64, 72, 80)), banded((120, 0, 8))
    tiny_near[0:SIDE, :] = jnp.where(even, lower, upper)
    tiny_far[0:SIDE, :] = jnp.where(even, upper, lower)
    for copy in edges:
        copy.wait()
    for offset, half, side, distance in corner_cells():
        count = 4 - distance
        at = SIDE + offset
        columns = slice(8 - count, 8) if side else slice(0, count)
        tiny_near[at : at + count, :] = edge[side, half, jnp.where(even, SIDE - distance, distance - 1), columns, :]
        tiny_far[at : at + count, :] = edge[side, half, jnp.where(even, distance - 1, SIDE - distance), columns, :]
    for side, message in enumerate((to_left, to_right)):
        for half in range(2):
            for row in range(SIDE):
                base = (half * SIDE + row) * 4
                message[base : base + 4, :] = edge[side, half, row, side * 4 : side * 4 + 4, :]
    for copy in tops:
        copy.wait()


def put_conductances(message, base, te, ts, tx, first_east, first_other):
    message[base : base + 5, :] = te[first_east : first_east + 5, :]
    message[base + 5 : base + 9, :] = ts[first_other : first_other + 4, :]
    message[base + 9 : base + 13, :] = tx[first_other : first_other + 4, :]
    message[base + 13 : base + 16, :] = jnp.zeros((3, 128), F32)


def first_kernel(te, ts, tx, load, s, x1, coef, factors):
    own = range(8, SIDE + 8, 8)
    turn_factors(te, ts, tx, factors, own, own, own)

    def body(group, carry):
        for step in range(8):
            row = group * 8 + 4 + step
            for c in own:
                signed = set_factors(coef, row, all_at(c), factors, 8 + step)
                root = jnp.abs(signed)
                supply = jnp.where(signed < 0.0, PAD_GAIN, 0.0)
                for half in range(2):
                    drawn = load[row - 4, c - 8 : c, half * 128 : half * 128 + 128]
                    s[half, row, c : c + 8, :] = (supply - drawn) * root
        for c in own:
            neighbours(s, coef, group * 8 + 3, 8, c, adding(x1))
            for which in range(3):
                factors[which, c : c + 8, :] = pltpu.roll(factors[which, c : c + 8, :], 120, 1)
        return carry

    lax.fori_loop(0, SIDE // 8, body, 0)


def corner_kernel(te, ts, tx, near, far, right, left, to_right, to_left, te2, ts2, tx2):
    lane = lanes_of((SIDE, 128))
    even = even_row()
    upper = jnp.where(even, far[0:SIDE, :], near[0:SIDE, :])
    lower = jnp.where(even, near[0:SIDE, :], far[0:SIDE, :])
    for source, target, down, up in ((te, te2, 0, 72), (ts, ts2, 120, 64), (tx, tx2, 112, 56)):
        head = pltpu.roll(upper, down, 1) if down else upper
        tail = pltpu.roll(lower, up, 1)
        own = source[8 : SIDE + 8, :]
        target[0:8, :] = jnp.zeros((8, 128), F32)
        target[8 : SIDE + 8, :] = jnp.where(lane < 8, head, jnp.where(lane < SIDE + 8, own, tail))
        target[SIDE + 8 :, :] = jnp.zeros((16, 128), F32)
    to_right[0:MAIN_MSG, :] = right[...]
    to_left[0:MAIN_MSG, :] = left[...]
    for offset, half, below, distance in corner_cells():
        count = 4 - distance
        for side, message in enumerate((to_left, to_right)):
            at = SIDE + (half * 2 + side) * 6 + (0, 3, 5)[distance - 1]
            first, second = (near, far) if below else (far, near)
            message[MAIN_MSG + offset : MAIN_MSG + offset + count, :] = jnp.where(
                even, first[at : at + count, :], second[at : at + count, :]
            )
    put_conductances(to_right, MAIN_MSG + 24, te2, ts2, tx2, SIDE + 3, SIDE + 4)
    put_conductances(to_left, MAIN_MSG + 24, te2, ts2, tx2, 8, 8)


def main_kernel(te, ts, tx, near, far, own_near, own_far, *rest):
    s, x1, coef, u, t, done, factors = rest[3:]
    even = even_row()
    own = range(8, SIDE + 8, 8)
    turn_factors(te, ts, tx, factors, own, own, own)
    for half in range(2):
        for row in range(4):
            at = (half * 4 + row) * SIDE
            one, other = near[at : at + SIDE, :], far[at : at + SIDE, :]
            s[half, row, 8 : SIDE + 8, :] = jnp.where(even, other, one)
            s[half, SIDE + 4 + row, 8 : SIDE + 8, :] = jnp.where(even, one, other)
        at = half * 4 * SIDE
        s[half, 4, 8 : SIDE + 8, :] = jnp.where(even, own_far[at : at + SIDE, :], own_near[at : at + SIDE, :])
    for row in (0, 1, 2, 3, 4, SIDE + 3, SIDE + 4, SIDE + 5, SIDE + 6, SIDE + 7):
        for c in own:
            signed = set_factors(coef, row, all_at(c), factors, row + 4)
            if row != SIDE + 3:
                to_source(s, row, c, signed)
    sweep(s, coef, 1, 6, own, 5, adding(x1))
    sweep(s, coef, SIDE + 3, SIDE + 7, own, 4, adding(x1))
    sweep(x1, coef, 2, SIDE + 6, own, 17, placing(u))
    sweep(u, coef, 3, SIDE + 5, own, 22, placing(t))

    def finish(half, row, c, total, here):
        done[half, row - 4, c - 8 : c, :] = result(s, u, coef, half, row, c, total)

    sweep(t, coef, 4, SIDE + 4, range(16, SIDE, 8), 16, finish)


def side_kernel(side, *refs):
    te2, ts2, tx2, message = refs[:4]
    s, x1, coef, u, t, out, done, te, ts, tx, factors, sem = refs[-12:]
    ready = refs[4 if side else 7]
    first, width = (0, 8) if side else (8, SIDE - 16)
    outs = []
    for half in range(2):
        copy = pltpu.make_async_copy(
            ready.at[half] if side else ready.at[half, :, pl.ds(8, width), :],
            out.at[:, pl.ds(first, width), pl.ds(half * 128, 128)],
            sem.at[4, half],
        )
        copy.start()
        outs.append(copy)
    for source, target in ((te2, te), (ts2, ts), (tx2, tx)):
        target[...] = source[...]
    at = MAIN_MSG + 24
    first_east, first_other = (SIDE + 8, SIDE + 8) if side else (3, 4)
    te[first_east : first_east + 5, :] = message[at : at + 5, :]
    ts[first_other : first_other + 4, :] = message[at + 5 : at + 9, :]
    tx[first_other : first_other + 4, :] = message[at + 9 : at + 13, :]
    c = SIDE + 8 if side else 1
    places = [(EAST, SIDE + 7 if side else 1), (SOUTH, c), (ROOT, c)]
    turn_factors(te, ts, tx, factors, (SIDE, c) if side else (c, 8), (places[0][1],), (c,))
    halo = SIDE + 8 if side else 4
    for row in range(SIDE):
        for half in range(2):
            at = (half * SIDE + row) * 4
            s[half, row + 4, halo : halo + 4, :] = message[at : at + 4, :]
            if side == 0:
                s[half, row + 4, 8:9, :] = refs[4][at : at + 1, :]
    if side == 0:
        even = even_row()
        for half in range(2):
            for row in range(4):
                at = (half * 4 + row) * SIDE
                one, other = refs[5][at : at + 1, :], refs[6][at : at + 1, :]
                s[half, row, 8:9, :] = jnp.where(even, other, one)
                s[half, SIDE + 4 + row, 8:9, :] = jnp.where(even, one, other)
    for offset, half, below, distance in corner_cells():
        count = 4 - distance
        row = SIDE + 3 + distance if below else 4 - distance
        start = SIDE + 8 if side else 8 - count
        s[half, row, start : start + count, :] = message[MAIN_MSG + offset : MAIN_MSG + offset + count, :]

    window = SIDE + 4 if side else 4

    def factor_rows(base):
        for step in range(8):
            to_source(s, base + step, c, set_factors(coef, base + step, places, factors, 4 + step))
        for which, k in places:
            factors[which, k : k + 8, :] = pltpu.roll(factors[which, k : k + 8, :], 120, 1)

    def body(group, carry):
        factor_rows(group * 8)
        neighbours(s, coef, group * 8 - 1, 8, window, adding(x1))
        return carry

    factor_rows(0)
    neighbours(s, coef, 1, 6, window, adding(x1))
    lax.fori_loop(1, ROWS // 8, body, 0)
    sweep(x1, coef, 2, SIDE + 6, (SIDE + 3 if side else 5,), 17, placing(u))
    sweep(u, coef, 3, SIDE + 5, (SIDE + 2 if side else 6,), 22, placing(t))

    def finish(half, row, c, total, here):
        done[half, row - 4, :, :] = result(s, u, coef, half, row, c, total)

    for part in range(4):
        rows = pl.ds(part * 16, 16)
        sweep(t, coef, 4 + part * 16, 20 + part * 16, (SIDE if side else 8,), 16, finish)
        for half in range(2):
            if side:
                copy = pltpu.make_async_copy(
                    done.at[half, rows],
                    out.at[rows, pl.ds(SIDE - 8, 8), pl.ds(half * 128, 128)],
                    sem.at[part, half],
                )
                copy.start()
                outs.append(copy)
    for copy in outs:
        copy.wait()


VMEM = pl.BlockSpec(memory_space=pltpu.VMEM)
HBM = pl.BlockSpec(memory_space=pltpu.HBM)
DMA = pltpu.SemaphoreType.DMA
FIELD = pltpu.VMEM((2, ROWS, COLS, 128), F32)
COEF = pltpu.VMEM((3, ROWS, COLS, 128), F32)
TURNED = pltpu.VMEM((TURNED_ROWS, 128), F32)
FACTORS = pltpu.VMEM((3, TURNED_ROWS, 128), F32)


def call(kernel, in_specs, out_shape, out_specs, scratch, cost, grant, aliases=None):
    return pl.pallas_call(
        kernel,
        in_specs=in_specs,
        out_shape=out_shape,
        out_specs=out_specs,
        scratch_shapes=scratch,
        input_output_aliases=aliases or {},
        cost_estimate=pl.CostEstimate(flops=cost, bytes_accessed=1 << 20, transcendentals=0),
        compiler_params=pltpu.CompilerParams(vmem_limit_bytes=grant << 20),
    )


def exchange(near, far):
    count = lax.axis_size("gx")
    far = lax.ppermute(far, "gx", [(i, (i - 1 + 2 * (i % 2)) % count) for i in range(count)])
    near = lax.ppermute(near, "gx", [(i, i ^ 1) for i in range(count)])
    return near, far


def block(east_class, south_class, cond_table, leakage, pad_mask, load):
    def shift(values, step):
        count = lax.axis_size("gy")
        return lax.ppermute(values, "gy", [(i, (i + step) % count) for i in range(count)])

    potential = pltpu.HBM((SIDE, SIDE, 256), F32)
    given = [pltpu.with_memory_space_constraint(a, pltpu.HBM) for a in (cond_table, east_class, south_class, leakage, pad_mask, load)]
    right, left, to_near, to_far, tiny_near, tiny_far, te, ts, tx = call(
        pack_kernel,
        [HBM] * 6,
        [pltpu.VMEM((MAIN_MSG, 128), F32)] * 4 + [pltpu.VMEM((TINY_MSG, 128), F32)] * 2 + [TURNED] * 3,
        [VMEM] * 9,
        [pltpu.SMEM((8,), F32)]
        + [pltpu.VMEM((SIDE, SIDE), kind) for kind in (jnp.int32, jnp.int32, F32, jnp.int32)]
        + [pltpu.VMEM((2, 2, SIDE, 8, 128), F32), DMA((2, 2)), DMA((2, 2, 4)), DMA((5,))],
        1 << 22,
        4,
    )(*given)
    late = lax.optimization_barrier((load, te))[0]
    tiny_one, tiny_other = exchange(tiny_near, tiny_far)
    one, other = exchange(to_near, to_far)
    to_right, to_left, te2, ts2, tx2 = call(
        corner_kernel, [VMEM] * 7, [pltpu.VMEM((FULL_MSG, 128), F32)] * 2 + [TURNED] * 3, [VMEM] * 5, [], 1 << 20, 4
    )(te, ts, tx, tiny_one, tiny_other, right, left)
    from_left = shift(to_right, 1)
    from_right = shift(to_left, -1)
    s, x1, coef = call(
        first_kernel, [VMEM] * 4, [FIELD, FIELD, COEF], [VMEM] * 3, [FACTORS], 1 << 25, 4
    )(te, ts, tx, pltpu.with_memory_space_constraint(late, pltpu.VMEM))
    *state, middle = call(
        main_kernel,
        [VMEM] * 10,
        [FIELD, FIELD, COEF, FIELD, FIELD, pltpu.VMEM((2, SIDE, SIDE, 128), F32)],
        [VMEM] * 6,
        [FACTORS],
        1 << 25,
        4,
        {7 + i: i for i in range(3)},
    )(te2, ts2, tx2, one, other, to_near, to_far, s, x1, coef)
    strip = pltpu.VMEM((2, SIDE, 8, 128), F32)
    *state, out, left_strip = call(
        functools.partial(side_kernel, 0),
        [VMEM] * 13,
        [FIELD, FIELD, COEF, FIELD, FIELD, potential, strip],
        [VMEM] * 5 + [HBM, VMEM],
        [TURNED] * 3 + [FACTORS, DMA((5, 2))],
        1 << 23,
        4,
        {8 + i: i for i in range(5)},
    )(te2, ts2, tx2, from_left, left, one, other, middle, *state)
    *state, out = call(
        functools.partial(side_kernel, 1),
        [VMEM] * 10 + [HBM],
        [FIELD, FIELD, COEF, FIELD, FIELD, potential],
        [VMEM] * 5 + [HBM],
        [strip] + [TURNED] * 3 + [FACTORS, DMA((5, 2))],
        1 << 23,
        4,
        {5 + i: i for i in range(6)},
    )(te2, ts2, tx2, from_right, left_strip, *state, out)
    return out


def solution(mesh):
    in_specs = (P("gx", "gy"), P("gx", "gy"), P(), P("gx", "gy"), P("gx", "gy"), P("gx", "gy", None))
    return jax.shard_map(block, mesh=mesh, in_specs=in_specs, out_specs=P("gx", "gy", None), check_vma=False)
```

```python
import functools

import jax
import jax.numpy as jnp
from jax import lax
from jax.experimental import pallas as pl
from jax.experimental.pallas import tpu as pltpu
from jax.sharding import PartitionSpec as P


PAD_GAIN = 8.0
SPECTRAL_BOUND = 0.995


SIDE = 64
ROWS = SIDE + 8
COLS = SIDE + 16
MAIN_MSG = 8 * SIDE
TINY_MSG = 16 + 24
FULL_MSG = MAIN_MSG + 24 + 16
TURNED_ROWS = SIDE + 24
F32 = jnp.float32


def weights():
    b2 = SPECTRAL_BOUND * SPECTRAL_BOUND
    first = 1.0 / (1.0 - b2 / 2.0)
    second = 1.0 / (1.0 - b2 * first / 4.0)
    third = 1.0 / (1.0 - b2 * second / 4.0)
    return first, second, third


W1, W2, W3 = weights()
MIX = W3 + (1.0 - W3) * W1
TOP = W1 * W2 * W3


EAST, SOUTH, ROOT = range(3)


def lanes_of(shape):
    return lax.broadcasted_iota(jnp.int32, shape, 1)


def turn_factors(te, ts, tx, factors, roots, easts, souths):
    for k in roots:
        south = ts[k : k + 8, :]
        ground = tx[k : k + 8, :]
        diagonal = te[k : k + 8, :] + te[k - 1 : k + 7, :] + south + pltpu.roll(south, 1, 1) + ground
        root = 1.0 / jnp.sqrt(diagonal)
        factors[ROOT, k : k + 8, :] = jnp.where(ground > 4.0, -root, root)
    for k in easts:
        factors[EAST, k : k + 8, :] = te[k : k + 8, :] * jnp.abs(factors[ROOT, k : k + 8, :] * factors[ROOT, k + 1 : k + 9, :])
    for k in souths:
        root = jnp.abs(factors[ROOT, k : k + 8, :])
        factors[SOUTH, k : k + 8, :] = ts[k : k + 8, :] * root * pltpu.roll(root, 127, 1)


def spread(values, lane):
    return jnp.broadcast_to(values[:, lane : lane + 1], (8, 128))


def set_factors(coef, row, places, factors, lane):
    for which, c in places:
        value = spread(factors[which, c : c + 8, :], lane)
        coef[which, row, c : c + 8, :] = jnp.abs(value) if which == ROOT else value
    return value


def to_source(s, row, c, signed):
    root = jnp.abs(signed)
    supply = jnp.where(signed < 0.0, PAD_GAIN, 0.0)
    for half in range(2):
        s[half, row, pl.ds(c, 8), :] = (supply - s[half, row, pl.ds(c, 8), :]) * root


def all_at(c):
    return [(EAST, c), (SOUTH, c), (ROOT, c)]


def neighbours(src, coef, base, count, c, emit):
    above = [src[half, base - 1, pl.ds(c, 8), :] for half in range(2)]
    here = [src[half, base, pl.ds(c, 8), :] for half in range(2)]
    north = coef[SOUTH, base - 1, pl.ds(c, 8), :]
    for step in range(count):
        row = base + step
        east = coef[EAST, row, pl.ds(c, 8), :]
        west = coef[EAST, row, pl.ds(c - 1, 8), :]
        south = coef[SOUTH, row, pl.ds(c, 8), :]
        for half in range(2):
            below = src[half, row + 1, pl.ds(c, 8), :]
            total = east * src[half, row, pl.ds(c + 1, 8), :] + west * src[half, row, pl.ds(c - 1, 8), :]
            total = total + (south * below + north * above[half])
            emit(half, row, c, total, here[half])
            above[half], here[half] = here[half], below
        north = south


def sweep(src, coef, first, last, columns, unroll, emit):
    full = (last - first) // unroll
    for c in columns:
        if full == 1:
            neighbours(src, coef, first, unroll, c, emit)
        elif full > 1:

            def trip(index, carry, c=c):
                neighbours(src, coef, first + index * unroll, unroll, c, emit)
                return carry

            lax.fori_loop(0, full, trip, 0)
        if first + full * unroll < last:
            neighbours(src, coef, first + full * unroll, last - first - full * unroll, c, emit)


def adding(target):
    def emit(half, row, c, total, here):
        target[half, row, pl.ds(c, 8), :] = here + total

    return emit


def placing(target):
    def emit(half, row, c, total, here):
        target[half, row, pl.ds(c, 8), :] = total

    return emit


def result(s, u, coef, half, row, c, total):
    value = s[half, row, pl.ds(c, 8), :] + (MIX * u[half, row, pl.ds(c, 8), :] + TOP * total)
    return value * coef[ROOT, row, pl.ds(c, 8), :]


def even_row():
    return lax.rem(lax.axis_index("gx"), 2) == 0


def corner_cells():
    for half in range(2):
        for side in range(2):
            for distance in (1, 2, 3):
                yield (half * 2 + side) * 6 + (0, 3, 5)[distance - 1], half, side, distance


def pack_kernel(*refs):
    small, load = refs[:5], refs[5]
    to_right, to_left, to_near, to_far, tiny_near, tiny_far, te, ts, tx = refs[6:15]
    even = even_row()
    near, far = jnp.where(even, SIDE - 4, 0), jnp.where(even, 0, SIDE - 4)
    edge, sem_edge, sem_rows, sem_small = refs[20:]
    table, east_class, south_class, leakage, pad_mask = refs[15:20]
    edges, tops = [], []
    nodes = [pltpu.make_async_copy(source, target, sem_small.at[i]) for i, (source, target) in enumerate(zip(small, refs[15:20]))]
    for copy in nodes:
        copy.start()
    for side in range(2):
        copy = pltpu.make_async_copy(load.at[:, pl.ds(side * (SIDE - 8), 8), :], edge.at[side], sem_edge.at[side])
        copy.start()
        edges.append(copy)
    for place, (start, message) in enumerate(((near, to_near), (far, to_far))):
        copy = pltpu.make_async_copy(load.at[pl.ds(start, 4)], message.at[pl.ds(0, 4)], sem_rows.at[place])
        copy.start()
        tops.append(copy)
    for copy in nodes:
        copy.wait()

    def look_up(classes):
        found = jnp.zeros((SIDE, SIDE), F32)
        for label in range(8):
            found = jnp.where(classes == label, table[label], found)
        return found

    zeros = jnp.zeros((SIDE, 128 - SIDE), F32)

    def turned(values):
        return pltpu.roll(jnp.concatenate([values.T, zeros], axis=1), 8, 1)

    east = turned(look_up(east_class[...]))
    south = turned(look_up(south_class[...]))
    ground = turned(leakage[...] + PAD_GAIN * pad_mask[...].astype(F32))
    for target, values in ((te, east), (ts, south), (tx, ground)):
        target[0:8, :] = jnp.zeros((8, 128), F32)
        target[8 : SIDE + 8, :] = values
        target[SIDE + 8 :, :] = jnp.zeros((16, 128), F32)
    lane = lanes_of((SIDE, 128))

    def banded(shifts):
        first, second, third = [
            values if shift == 0 else pltpu.roll(values, shift, 1) for values, shift in zip((east, south, ground), shifts)
        ]
        return jnp.where(lane < 8, first, jnp.where(lane < 16, second, third))

    lower, upper = banded((64, 72, 80)), banded((120, 0, 8))
    for tiny, message, banded_rows in (
        (tiny_near, to_near, jnp.where(even, lower, upper)),
        (tiny_far, to_far, jnp.where(even, upper, lower)),
    ):
        message[4, :, 0:128] = banded_rows
        message[4, :, 128:256] = jnp.zeros((SIDE, 128), F32)
        tiny[0:8, :] = banded_rows[0:8, :]
        tiny[8:16, :] = banded_rows[SIDE - 8 :, :]
    for copy in edges:
        copy.wait()
    for offset, half, side, distance in corner_cells():
        count = 4 - distance
        at = 16 + offset
        lanes = slice(half * 128, half * 128 + 128)
        columns = slice(8 - count, 8) if side else slice(0, count)
        tiny_near[at : at + count, :] = edge[side, jnp.where(even, SIDE - distance, distance - 1), columns, lanes]
        tiny_far[at : at + count, :] = edge[side, jnp.where(even, distance - 1, SIDE - distance), columns, lanes]
    for side, message in enumerate((to_left, to_right)):
        for half in range(2):
            for row in range(SIDE):
                base = (half * SIDE + row) * 4
                message[base : base + 4, :] = edge[side, row, side * 4 : side * 4 + 4, half * 128 : half * 128 + 128]
    for copy in tops:
        copy.wait()


def put_conductances(message, base, te, ts, tx, first_east, first_other):
    message[base : base + 5, :] = te[first_east : first_east + 5, :]
    message[base + 5 : base + 9, :] = ts[first_other : first_other + 4, :]
    message[base + 9 : base + 13, :] = tx[first_other : first_other + 4, :]
    message[base + 13 : base + 16, :] = jnp.zeros((3, 128), F32)


def first_kernel(te, ts, tx, load, s, x1, coef, factors):
    own = range(8, SIDE + 8, 8)
    turn_factors(te, ts, tx, factors, own, own, own)

    def body(group, carry):
        for step in range(8):
            row = group * 8 + 4 + step
            for c in own:
                signed = set_factors(coef, row, all_at(c), factors, 8 + step)
                root = jnp.abs(signed)
                supply = jnp.where(signed < 0.0, PAD_GAIN, 0.0)
                for half in range(2):
                    drawn = load[row - 4, c - 8 : c, half * 128 : half * 128 + 128]
                    s[half, row, c : c + 8, :] = (supply - drawn) * root
        for c in own:
            neighbours(s, coef, group * 8 + 3, 8, c, adding(x1))
            for which in range(3):
                factors[which, c : c + 8, :] = pltpu.roll(factors[which, c : c + 8, :], 120, 1)
        return carry

    lax.fori_loop(0, SIDE // 8, body, 0)


def widen(te, ts, tx, first, count, upper, lower):
    lane = lanes_of((count, 128))
    for target, down, up in ((te, 0, 72), (ts, 120, 64), (tx, 112, 56)):
        head = pltpu.roll(upper, down, 1) if down else upper
        own = target[first : first + count, :]
        target[first : first + count, :] = jnp.where(
            lane < 8, head, jnp.where(lane < SIDE + 8, own, pltpu.roll(lower, up, 1))
        )


def corner_kernel(te, ts, tx, near, far, right, left, to_right, to_left, te2, ts2, tx2):
    even = even_row()
    for source, target in ((te, te2), (ts, ts2), (tx, tx2)):
        target[...] = source[...]
    for at, first in ((0, 8), (8, SIDE)):
        one, other = near[at : at + 8, :], far[at : at + 8, :]
        widen(te2, ts2, tx2, first, 8, jnp.where(even, other, one), jnp.where(even, one, other))
    to_right[0:MAIN_MSG, :] = right[...]
    to_left[0:MAIN_MSG, :] = left[...]
    for offset, half, below, distance in corner_cells():
        count = 4 - distance
        for side, message in enumerate((to_left, to_right)):
            at = 16 + (half * 2 + side) * 6 + (0, 3, 5)[distance - 1]
            first, second = (near, far) if below else (far, near)
            message[MAIN_MSG + offset : MAIN_MSG + offset + count, :] = jnp.where(
                even, first[at : at + count, :], second[at : at + count, :]
            )
    put_conductances(to_right, MAIN_MSG + 24, te2, ts2, tx2, SIDE + 3, SIDE + 4)
    put_conductances(to_left, MAIN_MSG + 24, te2, ts2, tx2, 8, 8)


def main_kernel(own_te, own_ts, own_tx, near, far, own_near, own_far, *rest):
    s, x1, coef, u, t, done, te, ts, tx, factors = rest[3:]
    even = even_row()
    for source, target in ((own_te, te), (own_ts, ts), (own_tx, tx)):
        target[...] = source[...]
    one, other = near[4, :, 0:128], far[4, :, 0:128]
    widen(te, ts, tx, 8, SIDE, jnp.where(even, other, one), jnp.where(even, one, other))
    own = range(8, SIDE + 8, 8)
    turn_factors(te, ts, tx, factors, own, own, own)
    for half in range(2):
        for row in range(4):
            lanes = slice(half * 128, half * 128 + 128)
            one, other = near[row, :, lanes], far[row, :, lanes]
            s[half, row, 8 : SIDE + 8, :] = jnp.where(even, other, one)
            s[half, SIDE + 4 + row, 8 : SIDE + 8, :] = jnp.where(even, one, other)
        s[half, 4, 8 : SIDE + 8, :] = jnp.where(even, own_far[0, :, lanes], own_near[0, :, lanes])
    for row in (0, 1, 2, 3, 4, SIDE + 3, SIDE + 4, SIDE + 5, SIDE + 6, SIDE + 7):
        for c in own:
            signed = set_factors(coef, row, all_at(c), factors, row + 4)
            if row != SIDE + 3:
                to_source(s, row, c, signed)
    sweep(s, coef, 1, 6, own, 5, adding(x1))
    sweep(s, coef, SIDE + 3, SIDE + 7, own, 4, adding(x1))
    sweep(x1, coef, 2, SIDE + 6, own, 17, placing(u))
    sweep(u, coef, 3, SIDE + 5, own, 22, placing(t))

    def finish(half, row, c, total, here):
        done[half, row - 4, c - 8 : c, :] = result(s, u, coef, half, row, c, total)

    sweep(t, coef, 4, SIDE + 4, range(16, SIDE, 8), 16, finish)


def side_kernel(side, *refs):
    te2, ts2, tx2, message = refs[:4]
    s, x1, coef, u, t, out, done, te, ts, tx, factors, sem = refs[-12:]
    middle = refs[4 if side else 7]
    outs = [
        pltpu.make_async_copy(
            middle.at[side, :, pl.ds(8, SIDE - 16), :],
            out.at[:, pl.ds(8, SIDE - 16), pl.ds(side * 128, 128)],
            sem.at[4, 0],
        )
    ]
    if side:
        for half in range(2):
            outs.append(
                pltpu.make_async_copy(
                    refs[5].at[half], out.at[:, pl.ds(0, 8), pl.ds(half * 128, 128)], sem.at[4, 1 + half]
                )
            )
    for copy in outs:
        copy.start()
    for source, target in ((te2, te), (ts2, ts), (tx2, tx)):
        target[...] = source[...]
    at = MAIN_MSG + 24
    first_east, first_other = (SIDE + 8, SIDE + 8) if side else (3, 4)
    te[first_east : first_east + 5, :] = message[at : at + 5, :]
    ts[first_other : first_other + 4, :] = message[at + 5 : at + 9, :]
    tx[first_other : first_other + 4, :] = message[at + 9 : at + 13, :]
    c = SIDE + 8 if side else 1
    places = [(EAST, SIDE + 7 if side else 1), (SOUTH, c), (ROOT, c)]
    turn_factors(te, ts, tx, factors, (SIDE, c) if side else (c, 8), (places[0][1],), (c,))
    halo = SIDE + 8 if side else 4
    for row in range(SIDE):
        for half in range(2):
            at = (half * SIDE + row) * 4
            s[half, row + 4, halo : halo + 4, :] = message[at : at + 4, :]
            if side == 0:
                s[half, row + 4, 8:9, :] = refs[4][at : at + 1, :]
    if side == 0:
        even = even_row()
        for half in range(2):
            for row in range(4):
                lanes = slice(half * 128, half * 128 + 128)
                one, other = refs[5][row, 0:1, lanes], refs[6][row, 0:1, lanes]
                s[half, row, 8:9, :] = jnp.where(even, other, one)
                s[half, SIDE + 4 + row, 8:9, :] = jnp.where(even, one, other)
    for offset, half, below, distance in corner_cells():
        count = 4 - distance
        row = SIDE + 3 + distance if below else 4 - distance
        start = SIDE + 8 if side else 8 - count
        s[half, row, start : start + count, :] = message[MAIN_MSG + offset : MAIN_MSG + offset + count, :]

    window = SIDE + 4 if side else 4

    for group in range(ROWS // 8):
        for row in range(group * 8, group * 8 + 8):
            to_source(s, row, c, set_factors(coef, row, places, factors, row + 4))
        if group == 0:
            neighbours(s, coef, 1, 6, window, adding(x1))
        else:
            neighbours(s, coef, group * 8 - 1, 8, window, adding(x1))
    sweep(x1, coef, 2, SIDE + 6, (SIDE + 3 if side else 5,), 34, placing(u))
    sweep(u, coef, 3, SIDE + 5, (SIDE + 2 if side else 6,), 33, placing(t))

    def finish(half, row, c, total, here):
        done[half, row - 4, :, :] = result(s, u, coef, half, row, c, total)

    for part in range(4):
        rows = pl.ds(part * 16, 16)
        sweep(t, coef, 4 + part * 16, 20 + part * 16, (SIDE if side else 8,), 16, finish)
        for half in range(2):
            if side:
                copy = pltpu.make_async_copy(
                    done.at[half, rows],
                    out.at[rows, pl.ds(SIDE - 8, 8), pl.ds(half * 128, 128)],
                    sem.at[part, half],
                )
                copy.start()
                outs.append(copy)
    for copy in outs:
        copy.wait()


VMEM = pl.BlockSpec(memory_space=pltpu.VMEM)
HBM = pl.BlockSpec(memory_space=pltpu.HBM)
DMA = pltpu.SemaphoreType.DMA
FIELD = pltpu.VMEM((2, ROWS, COLS, 128), F32)
COEF = pltpu.VMEM((3, ROWS, COLS, 128), F32)
TURNED = pltpu.VMEM((TURNED_ROWS, 128), F32)
FACTORS = pltpu.VMEM((3, TURNED_ROWS, 128), F32)


def call(kernel, in_specs, out_shape, out_specs, scratch, cost, grant, aliases=None):
    return pl.pallas_call(
        kernel,
        in_specs=in_specs,
        out_shape=out_shape,
        out_specs=out_specs,
        scratch_shapes=scratch,
        input_output_aliases=aliases or {},
        cost_estimate=pl.CostEstimate(flops=cost, bytes_accessed=1 << 20, transcendentals=0),
        compiler_params=pltpu.CompilerParams(vmem_limit_bytes=grant << 20),
    )


def exchange(near, far):
    count = lax.axis_size("gx")
    far = lax.ppermute(far, "gx", [(i, (i - 1 + 2 * (i % 2)) % count) for i in range(count)])
    near = lax.ppermute(near, "gx", [(i, i ^ 1) for i in range(count)])
    return near, far


def block(east_class, south_class, cond_table, leakage, pad_mask, load):
    def shift(values, step):
        count = lax.axis_size("gy")
        return lax.ppermute(values, "gy", [(i, (i + step) % count) for i in range(count)])

    potential = pltpu.HBM((SIDE, SIDE, 256), F32)
    given = [pltpu.with_memory_space_constraint(a, pltpu.HBM) for a in (cond_table, east_class, south_class, leakage, pad_mask, load)]
    right, left, to_near, to_far, tiny_near, tiny_far, te, ts, tx = call(
        pack_kernel,
        [HBM] * 6,
        [pltpu.VMEM((MAIN_MSG, 128), F32)] * 2 + [pltpu.VMEM((5, SIDE, 256), F32)] * 2 + [pltpu.VMEM((TINY_MSG, 128), F32)] * 2 + [TURNED] * 3,
        [VMEM] * 9,
        [pltpu.SMEM((8,), F32)]
        + [pltpu.VMEM((SIDE, SIDE), kind) for kind in (jnp.int32, jnp.int32, F32, jnp.int32)]
        + [pltpu.VMEM((2, SIDE, 8, 256), F32), DMA((2,)), DMA((2,)), DMA((5,))],
        1 << 22,
        4,
    )(*given)
    late = lax.optimization_barrier((load, te))[0]
    tiny_one, tiny_other = exchange(tiny_near, tiny_far)
    one, other = exchange(to_near, to_far)
    to_right, to_left, te2, ts2, tx2 = call(
        corner_kernel, [VMEM] * 7, [pltpu.VMEM((FULL_MSG, 128), F32)] * 2 + [TURNED] * 3, [VMEM] * 5, [], 1 << 20, 4
    )(te, ts, tx, tiny_one, tiny_other, right, left)
    from_left = shift(to_right, 1)
    from_right = shift(to_left, -1)
    s, x1, coef = call(
        first_kernel, [VMEM] * 4, [FIELD, FIELD, COEF], [VMEM] * 3, [FACTORS], 1 << 25, 4
    )(te, ts, tx, pltpu.with_memory_space_constraint(late, pltpu.VMEM))
    *state, middle = call(
        main_kernel,
        [VMEM] * 10,
        [FIELD, FIELD, COEF, FIELD, FIELD, pltpu.VMEM((2, SIDE, SIDE, 128), F32)],
        [VMEM] * 6,
        [TURNED] * 3 + [FACTORS],
        1 << 25,
        4,
        {7 + i: i for i in range(3)},
    )(te, ts, tx, one, other, to_near, to_far, s, x1, coef)
    strip = pltpu.VMEM((2, SIDE, 8, 128), F32)
    *state, out, left_strip = call(
        functools.partial(side_kernel, 0),
        [VMEM] * 13,
        [FIELD, FIELD, COEF, FIELD, FIELD, potential, strip],
        [VMEM] * 5 + [HBM, VMEM],
        [TURNED] * 3 + [FACTORS, DMA((5, 3))],
        1 << 23,
        4,
        {8 + i: i for i in range(5)},
    )(te2, ts2, tx2, from_left, left, one, other, middle, *state)
    *state, out = call(
        functools.partial(side_kernel, 1),
        [VMEM] * 11 + [HBM],
        [FIELD, FIELD, COEF, FIELD, FIELD, potential],
        [VMEM] * 5 + [HBM],
        [strip] + [TURNED] * 3 + [FACTORS, DMA((5, 3))],
        1 << 23,
        4,
        {6 + i: i for i in range(6)},
    )(te2, ts2, tx2, from_right, middle, left_strip, *state, out)
    return out


def solution(mesh):
    in_specs = (P("gx", "gy"), P("gx", "gy"), P(), P("gx", "gy"), P("gx", "gy"), P("gx", "gy", None))
    return jax.shard_map(block, mesh=mesh, in_specs=in_specs, out_specs=P("gx", "gy", None), check_vma=False)
```

```python
import functools

import jax
import jax.numpy as jnp
from jax import lax
from jax.experimental import pallas as pl
from jax.experimental.pallas import tpu as pltpu
from jax.sharding import PartitionSpec as P


PAD_GAIN = 8.0
SPECTRAL_BOUND = 0.995


SIDE = 64
ROWS = SIDE + 8
COLS = SIDE + 16
MAIN_MSG = 8 * SIDE
TINY_MSG = 24 + 24
FULL_MSG = MAIN_MSG + 24 + 16
TURNED_ROWS = SIDE + 24
F32 = jnp.float32


def weights():
    b2 = SPECTRAL_BOUND * SPECTRAL_BOUND
    first = 1.0 / (1.0 - b2 / 2.0)
    second = 1.0 / (1.0 - b2 * first / 4.0)
    third = 1.0 / (1.0 - b2 * second / 4.0)
    return first, second, third


W1, W2, W3 = weights()
MIX = W3 + (1.0 - W3) * W1
TOP = W1 * W2 * W3


EAST, SOUTH, ROOT = range(3)


def lanes_of(shape):
    return lax.broadcasted_iota(jnp.int32, shape, 1)


def turn_factors(te, ts, tx, factors, roots, easts, souths):
    for k in roots:
        south = ts[k : k + 8, :]
        ground = tx[k : k + 8, :]
        diagonal = te[k : k + 8, :] + te[k - 1 : k + 7, :] + south + pltpu.roll(south, 1, 1) + ground
        root = 1.0 / jnp.sqrt(diagonal)
        factors[ROOT, k : k + 8, :] = jnp.where(ground > 4.0, -root, root)
    for k in easts:
        factors[EAST, k : k + 8, :] = te[k : k + 8, :] * jnp.abs(factors[ROOT, k : k + 8, :] * factors[ROOT, k + 1 : k + 9, :])
    for k in souths:
        root = jnp.abs(factors[ROOT, k : k + 8, :])
        factors[SOUTH, k : k + 8, :] = ts[k : k + 8, :] * root * pltpu.roll(root, 127, 1)


def spread(values, lane):
    return jnp.broadcast_to(values[:, lane : lane + 1], (8, 128))


def set_factors(coef, row, places, factors, lane):
    for which, c in places:
        value = spread(factors[which, c : c + 8, :], lane)
        coef[which, row, c : c + 8, :] = jnp.abs(value) if which == ROOT else value
    return value


def to_source(s, row, c, signed):
    root = jnp.abs(signed)
    supply = jnp.where(signed < 0.0, PAD_GAIN, 0.0)
    for half in range(2):
        s[half, row, pl.ds(c, 8), :] = (supply - s[half, row, pl.ds(c, 8), :]) * root


def all_at(c):
    return [(EAST, c), (SOUTH, c), (ROOT, c)]


def neighbours(src, coef, base, count, c, emit):
    above = [src[half, base - 1, pl.ds(c, 8), :] for half in range(2)]
    here = [src[half, base, pl.ds(c, 8), :] for half in range(2)]
    north = coef[SOUTH, base - 1, pl.ds(c, 8), :]
    for step in range(count):
        row = base + step
        east = coef[EAST, row, pl.ds(c, 8), :]
        west = coef[EAST, row, pl.ds(c - 1, 8), :]
        south = coef[SOUTH, row, pl.ds(c, 8), :]
        for half in range(2):
            below = src[half, row + 1, pl.ds(c, 8), :]
            total = east * src[half, row, pl.ds(c + 1, 8), :] + west * src[half, row, pl.ds(c - 1, 8), :]
            total = total + (south * below + north * above[half])
            emit(half, row, c, total, here[half])
            above[half], here[half] = here[half], below
        north = south


def sweep(src, coef, first, last, columns, unroll, emit):
    full = (last - first) // unroll
    for c in columns:
        if full == 1:
            neighbours(src, coef, first, unroll, c, emit)
        elif full > 1:

            def trip(index, carry, c=c):
                neighbours(src, coef, first + index * unroll, unroll, c, emit)
                return carry

            lax.fori_loop(0, full, trip, 0)
        if first + full * unroll < last:
            neighbours(src, coef, first + full * unroll, last - first - full * unroll, c, emit)


def adding(target):
    def emit(half, row, c, total, here):
        target[half, row, pl.ds(c, 8), :] = here + total

    return emit


def placing(target):
    def emit(half, row, c, total, here):
        target[half, row, pl.ds(c, 8), :] = total

    return emit


def result(s, u, coef, half, row, c, total):
    value = s[half, row, pl.ds(c, 8), :] + (MIX * u[half, row, pl.ds(c, 8), :] + TOP * total)
    return value * coef[ROOT, row, pl.ds(c, 8), :]


def even_row():
    return lax.rem(lax.axis_index("gx"), 2) == 0


def corner_cells():
    for half in range(2):
        for side in range(2):
            for distance in (1, 2, 3):
                yield (half * 2 + side) * 6 + (0, 3, 5)[distance - 1], half, side, distance


def pack_kernel(*refs):
    small, load = refs[:5], refs[5]
    to_right, to_left, to_near, to_far, tiny_near, tiny_far, te, ts, tx = refs[6:15]
    even = even_row()
    near, far = jnp.where(even, SIDE - 4, 0), jnp.where(even, 0, SIDE - 4)
    edge, sem_edge, sem_rows, sem_small = refs[20:]
    table, east_class, south_class, leakage, pad_mask = refs[15:20]
    edges, tops = [], []
    nodes = [pltpu.make_async_copy(source, target, sem_small.at[i]) for i, (source, target) in enumerate(zip(small, refs[15:20]))]
    for copy in nodes:
        copy.start()
    for side in range(2):
        copy = pltpu.make_async_copy(load.at[:, pl.ds(side * (SIDE - 8), 8), :], edge.at[side], sem_edge.at[side])
        copy.start()
        edges.append(copy)
    for place, (start, message) in enumerate(((near, to_near), (far, to_far))):
        copy = pltpu.make_async_copy(load.at[pl.ds(start, 4)], message, sem_rows.at[place])
        copy.start()
        tops.append(copy)
    for copy in nodes:
        copy.wait()

    def look_up(classes):
        found = jnp.zeros((SIDE, SIDE), F32)
        for label in range(8):
            found = jnp.where(classes == label, table[label], found)
        return found

    zeros = jnp.zeros((SIDE, 128 - SIDE), F32)
    nodes_of = (
        look_up(east_class[...]),
        look_up(south_class[...]),
        leakage[...] + PAD_GAIN * pad_mask[...].astype(F32),
    )
    for target, values in zip((te, ts, tx), nodes_of):
        target[0:8, :] = jnp.zeros((8, 128), F32)
        target[8 : SIDE + 8, :] = pltpu.roll(jnp.concatenate([values.T, zeros], axis=1), 8, 1)
        target[SIDE + 8 :, :] = jnp.zeros((16, 128), F32)
    for place, values in enumerate(nodes_of):
        head, tail = values[0:8, :], values[SIDE - 8 :, :]
        for tiny, edge_rows in ((tiny_near, jnp.where(even, tail, head)), (tiny_far, jnp.where(even, head, tail))):
            tiny[place * 8 : place * 8 + 8, :] = jnp.concatenate([edge_rows, zeros[0:8, :]], axis=1)
    for copy in edges:
        copy.wait()
    for offset, half, side, distance in corner_cells():
        count = 4 - distance
        at = 24 + offset
        lanes = slice(half * 128, half * 128 + 128)
        columns = slice(8 - count, 8) if side else slice(0, count)
        tiny_near[at : at + count, :] = edge[side, jnp.where(even, SIDE - distance, distance - 1), columns, lanes]
        tiny_far[at : at + count, :] = edge[side, jnp.where(even, distance - 1, SIDE - distance), columns, lanes]
    for side, message in enumerate((to_left, to_right)):
        for half in range(2):
            for row in range(SIDE):
                base = (half * SIDE + row) * 4
                message[base : base + 4, :] = edge[side, row, side * 4 : side * 4 + 4, half * 128 : half * 128 + 128]
    for copy in tops:
        copy.wait()


def put_conductances(message, base, te, ts, tx, first_east, first_other):
    message[base : base + 5, :] = te[first_east : first_east + 5, :]
    message[base + 5 : base + 9, :] = ts[first_other : first_other + 4, :]
    message[base + 9 : base + 13, :] = tx[first_other : first_other + 4, :]
    message[base + 13 : base + 16, :] = jnp.zeros((3, 128), F32)


def first_kernel(te, ts, tx, load, s, x1, coef, factors):
    own = range(8, SIDE + 8, 8)
    turn_factors(te, ts, tx, factors, own, own, own)

    def body(group, carry):
        for step in range(8):
            row = group * 8 + 4 + step
            for c in own:
                signed = set_factors(coef, row, all_at(c), factors, 8 + step)
                root = jnp.abs(signed)
                supply = jnp.where(signed < 0.0, PAD_GAIN, 0.0)
                for half in range(2):
                    drawn = load[row - 4, c - 8 : c, half * 128 : half * 128 + 128]
                    s[half, row, c : c + 8, :] = (supply - drawn) * root
        for c in own:
            neighbours(s, coef, group * 8 + 3, 8, c, adding(x1))
            for which in range(3):
                factors[which, c : c + 8, :] = pltpu.roll(factors[which, c : c + 8, :], 120, 1)
        return carry

    lax.fori_loop(0, SIDE // 8, body, 0)


def widen(te, ts, tx, upper, lower):
    lane = lanes_of((SIDE, 128))
    for target, down, up in ((te, 0, 72), (ts, 120, 64), (tx, 112, 56)):
        head = pltpu.roll(upper, down, 1) if down else upper
        own = target[8 : SIDE + 8, :]
        target[8 : SIDE + 8, :] = jnp.where(lane < 8, head, jnp.where(lane < SIDE + 8, own, pltpu.roll(lower, up, 1)))


def corner_kernel(te, ts, tx, near, far, right, left, to_right, to_left, te2, ts2, tx2):
    even = even_row()
    for source, target in ((te, te2), (ts, ts2), (tx, tx2)):
        target[...] = source[...]
    fill = jnp.zeros((104, 128), F32)
    one, other = [jnp.concatenate([tiny[0:24, :], fill], axis=0).T[0:SIDE, :] for tiny in (near, far)]
    widen(te2, ts2, tx2, jnp.where(even, other, one), jnp.where(even, one, other))
    to_right[0:MAIN_MSG, :] = right[...]
    to_left[0:MAIN_MSG, :] = left[...]
    for offset, half, below, distance in corner_cells():
        count = 4 - distance
        for side, message in enumerate((to_left, to_right)):
            at = 24 + (half * 2 + side) * 6 + (0, 3, 5)[distance - 1]
            first, second = (near, far) if below else (far, near)
            message[MAIN_MSG + offset : MAIN_MSG + offset + count, :] = jnp.where(
                even, first[at : at + count, :], second[at : at + count, :]
            )
    put_conductances(to_right, MAIN_MSG + 24, te2, ts2, tx2, SIDE + 3, SIDE + 4)
    put_conductances(to_left, MAIN_MSG + 24, te2, ts2, tx2, 8, 8)


def main_kernel(te, ts, tx, near, far, own_near, own_far, *rest):
    s, x1, coef, u, t, done, factors = rest[3:]
    even = even_row()
    own = range(8, SIDE + 8, 8)
    turn_factors(te, ts, tx, factors, own, own, own)
    for half in range(2):
        for row in range(4):
            lanes = slice(half * 128, half * 128 + 128)
            one, other = near[row, :, lanes], far[row, :, lanes]
            s[half, row, 8 : SIDE + 8, :] = jnp.where(even, other, one)
            s[half, SIDE + 4 + row, 8 : SIDE + 8, :] = jnp.where(even, one, other)
        s[half, 4, 8 : SIDE + 8, :] = jnp.where(even, own_far[0, :, lanes], own_near[0, :, lanes])
    for row in (0, 1, 2, 3, 4, SIDE + 3, SIDE + 4, SIDE + 5, SIDE + 6, SIDE + 7):
        for c in own:
            signed = set_factors(coef, row, all_at(c), factors, row + 4)
            if row != SIDE + 3:
                to_source(s, row, c, signed)
    sweep(s, coef, 1, 6, own, 5, adding(x1))
    sweep(s, coef, SIDE + 3, SIDE + 7, own, 4, adding(x1))
    sweep(x1, coef, 2, SIDE + 6, own, 17, placing(u))
    sweep(u, coef, 3, SIDE + 5, own, 22, placing(t))

    def finish(half, row, c, total, here):
        done[half, row - 4, c - 8 : c, :] = result(s, u, coef, half, row, c, total)

    sweep(t, coef, 4, SIDE + 4, range(16, SIDE, 8), 16, finish)


def side_kernel(side, *refs):
    te2, ts2, tx2, message = refs[:4]
    s, x1, coef, u, t, out, done, te, ts, tx, factors, sem = refs[-12:]
    middle = refs[4 if side else 7]
    outs = [
        pltpu.make_async_copy(
            middle.at[side, :, pl.ds(8, SIDE - 16), :],
            out.at[:, pl.ds(8, SIDE - 16), pl.ds(side * 128, 128)],
            sem.at[4, 0],
        )
    ]
    if side:
        for half in range(2):
            outs.append(
                pltpu.make_async_copy(
                    refs[5].at[half], out.at[:, pl.ds(0, 8), pl.ds(half * 128, 128)], sem.at[4, 1 + half]
                )
            )
    for copy in outs:
        copy.start()
    for source, target in ((te2, te), (ts2, ts), (tx2, tx)):
        target[...] = source[...]
    at = MAIN_MSG + 24
    first_east, first_other = (SIDE + 8, SIDE + 8) if side else (3, 4)
    te[first_east : first_east + 5, :] = message[at : at + 5, :]
    ts[first_other : first_other + 4, :] = message[at + 5 : at + 9, :]
    tx[first_other : first_other + 4, :] = message[at + 9 : at + 13, :]
    c = SIDE + 8 if side else 1
    places = [(EAST, SIDE + 7 if side else 1), (SOUTH, c), (ROOT, c)]
    turn_factors(te, ts, tx, factors, (SIDE, c) if side else (c, 8), (places[0][1],), (c,))
    halo = SIDE + 8 if side else 4
    for row in range(SIDE):
        for half in range(2):
            at = (half * SIDE + row) * 4
            s[half, row + 4, halo : halo + 4, :] = message[at : at + 4, :]
            if side == 0:
                s[half, row + 4, 8:9, :] = refs[4][at : at + 1, :]
    if side == 0:
        even = even_row()
        for half in range(2):
            for row in range(4):
                lanes = slice(half * 128, half * 128 + 128)
                one, other = refs[5][row, 0:1, lanes], refs[6][row, 0:1, lanes]
                s[half, row, 8:9, :] = jnp.where(even, other, one)
                s[half, SIDE + 4 + row, 8:9, :] = jnp.where(even, one, other)
    for offset, half, below, distance in corner_cells():
        count = 4 - distance
        row = SIDE + 3 + distance if below else 4 - distance
        start = SIDE + 8 if side else 8 - count
        s[half, row, start : start + count, :] = message[MAIN_MSG + offset : MAIN_MSG + offset + count, :]

    window = SIDE + 4 if side else 4

    for group in range(ROWS // 8):
        for row in range(group * 8, group * 8 + 8):
            to_source(s, row, c, set_factors(coef, row, places, factors, row + 4))
        if group == 0:
            neighbours(s, coef, 1, 6, window, adding(x1))
        else:
            neighbours(s, coef, group * 8 - 1, 8, window, adding(x1))
    sweep(x1, coef, 2, SIDE + 6, (SIDE + 3 if side else 5,), 34, placing(u))
    sweep(u, coef, 3, SIDE + 5, (SIDE + 2 if side else 6,), 33, placing(t))

    def finish(half, row, c, total, here):
        done[half, row - 4, :, :] = result(s, u, coef, half, row, c, total)

    for part in range(4):
        rows = pl.ds(part * 16, 16)
        sweep(t, coef, 4 + part * 16, 20 + part * 16, (SIDE if side else 8,), 16, finish)
        for half in range(2):
            if side:
                copy = pltpu.make_async_copy(
                    done.at[half, rows],
                    out.at[rows, pl.ds(SIDE - 8, 8), pl.ds(half * 128, 128)],
                    sem.at[part, half],
                )
                copy.start()
                outs.append(copy)
    for copy in outs:
        copy.wait()


VMEM = pl.BlockSpec(memory_space=pltpu.VMEM)
HBM = pl.BlockSpec(memory_space=pltpu.HBM)
DMA = pltpu.SemaphoreType.DMA
FIELD = pltpu.VMEM((2, ROWS, COLS, 128), F32)
COEF = pltpu.VMEM((3, ROWS, COLS, 128), F32)
TURNED = pltpu.VMEM((TURNED_ROWS, 128), F32)
FACTORS = pltpu.VMEM((3, TURNED_ROWS, 128), F32)


def call(kernel, in_specs, out_shape, out_specs, scratch, cost, grant, aliases=None):
    return pl.pallas_call(
        kernel,
        in_specs=in_specs,
        out_shape=out_shape,
        out_specs=out_specs,
        scratch_shapes=scratch,
        input_output_aliases=aliases or {},
        cost_estimate=pl.CostEstimate(flops=cost, bytes_accessed=1 << 20, transcendentals=0),
        compiler_params=pltpu.CompilerParams(vmem_limit_bytes=grant << 20),
    )


def exchange(near, far):
    count = lax.axis_size("gx")
    far = lax.ppermute(far, "gx", [(i, (i - 1 + 2 * (i % 2)) % count) for i in range(count)])
    near = lax.ppermute(near, "gx", [(i, i ^ 1) for i in range(count)])
    return near, far


def block(east_class, south_class, cond_table, leakage, pad_mask, load):
    def shift(values, step):
        count = lax.axis_size("gy")
        return lax.ppermute(values, "gy", [(i, (i + step) % count) for i in range(count)])

    potential = pltpu.HBM((SIDE, SIDE, 256), F32)
    given = [pltpu.with_memory_space_constraint(a, pltpu.HBM) for a in (cond_table, east_class, south_class, leakage, pad_mask, load)]
    right, left, to_near, to_far, tiny_near, tiny_far, te, ts, tx = call(
        pack_kernel,
        [HBM] * 6,
        [pltpu.VMEM((MAIN_MSG, 128), F32)] * 2 + [pltpu.VMEM((4, SIDE, 256), F32)] * 2 + [pltpu.VMEM((TINY_MSG, 128), F32)] * 2 + [TURNED] * 3,
        [VMEM] * 9,
        [pltpu.SMEM((8,), F32)]
        + [pltpu.VMEM((SIDE, SIDE), kind) for kind in (jnp.int32, jnp.int32, F32, jnp.int32)]
        + [pltpu.VMEM((2, SIDE, 8, 256), F32), DMA((2,)), DMA((2,)), DMA((5,))],
        1 << 22,
        4,
    )(*given)
    late = lax.optimization_barrier((load, te))[0]
    tiny_one, tiny_other = exchange(tiny_near, tiny_far)
    one, other = exchange(to_near, to_far)
    to_right, to_left, te2, ts2, tx2 = call(
        corner_kernel, [VMEM] * 7, [pltpu.VMEM((FULL_MSG, 128), F32)] * 2 + [TURNED] * 3, [VMEM] * 5, [], 1 << 20, 4
    )(te, ts, tx, tiny_one, tiny_other, right, left)
    from_left = shift(to_right, 1)
    from_right = shift(to_left, -1)
    s, x1, coef = call(
        first_kernel, [VMEM] * 4, [FIELD, FIELD, COEF], [VMEM] * 3, [FACTORS], 1 << 25, 4
    )(te, ts, tx, pltpu.with_memory_space_constraint(late, pltpu.VMEM))
    *state, middle = call(
        main_kernel,
        [VMEM] * 10,
        [FIELD, FIELD, COEF, FIELD, FIELD, pltpu.VMEM((2, SIDE, SIDE, 128), F32)],
        [VMEM] * 6,
        [FACTORS],
        1 << 25,
        4,
        {7 + i: i for i in range(3)},
    )(te2, ts2, tx2, one, other, to_near, to_far, s, x1, coef)
    strip = pltpu.VMEM((2, SIDE, 8, 128), F32)
    *state, out, left_strip = call(
        functools.partial(side_kernel, 0),
        [VMEM] * 13,
        [FIELD, FIELD, COEF, FIELD, FIELD, potential, strip],
        [VMEM] * 5 + [HBM, VMEM],
        [TURNED] * 3 + [FACTORS, DMA((5, 3))],
        1 << 23,
        4,
        {8 + i: i for i in range(5)},
    )(te2, ts2, tx2, from_left, left, one, other, middle, *state)
    *state, out = call(
        functools.partial(side_kernel, 1),
        [VMEM] * 11 + [HBM],
        [FIELD, FIELD, COEF, FIELD, FIELD, potential],
        [VMEM] * 5 + [HBM],
        [strip] + [TURNED] * 3 + [FACTORS, DMA((5, 3))],
        1 << 23,
        4,
        {6 + i: i for i in range(6)},
    )(te2, ts2, tx2, from_right, middle, left_strip, *state, out)
    return out


def solution(mesh):
    in_specs = (P("gx", "gy"), P("gx", "gy"), P(), P("gx", "gy"), P("gx", "gy"), P("gx", "gy", None))
    return jax.shard_map(block, mesh=mesh, in_specs=in_specs, out_specs=P("gx", "gy", None), check_vma=False)
```
